128 devices in a mesh: seq: 32 (over z, y_hi, x), head: 4 (over y_lo, core).
Axes of the slice: x: 4, y: 4 (y_hi: 2, y_lo: 2; y = y_hi * 2 + y_lo), z: 4, core: 2. Of those that a mesh axis runs over, the one named last changes fastest.
Arguments:
- queries: bfloat16 [8192, 3584], P('seq', 'head'), may hold values from -5 to 5
- keys: bfloat16 [8192, 3584], P('seq', 'head'), may hold values from -5 to 5
- values: bfloat16 [8192, 3584], P('seq', 'head'), may hold values from -6 to 6
- attn_grad: bfloat16 [8192, 3584], P('seq', 'head'), may hold values from -6 to 6
- doc_ids: int32 [8192], replicated, may hold values from 0 to 7, never falling along the last dimension, each value on 1 to 4096 neighbouring positions
- conv_input: bfloat16 [8192, 7168], P('seq', 'head'), may hold values from -6 to 6
- conv_weight: float32 [4, 7168], P(None, 'head'), may hold values from -3 to 3
- step_raw: float32 [8192, 112], P('seq', 'head'), may hold values from -4 to 4
- step_bias: float32 [112], P('head'), may hold values from -1.5 to 0
- rate_log: float32 [112], P('head'), may hold values from -13 to -1
- skip_gain: float32 [112], P('head'), may hold values from 0.5 to 1.5
- input_coeff: bfloat16 [8192, 128], P('seq'), may hold values from -0.625 to 0.625
- output_coeff: bfloat16 [8192, 128], P('seq'), may hold values from -0.625 to 0.625
- gate_input: bfloat16 [8192, 7168], P('seq', 'head'), may hold values from -6 to 6
- mix_grad: bfloat16 [8192, 7168], P('seq', 'head'), may hold values from -1.5 to 1.5
Outputs:
- grad_queries: bfloat16 [8192, 3584], P('seq', 'head')
- grad_keys: bfloat16 [8192, 3584], P('seq', 'head')
- grad_values: bfloat16 [8192, 3584], P('seq', 'head')
- grad_conv_input: bfloat16 [8192, 7168], P('seq', 'head')
- grad_gate: bfloat16 [8192, 7168], P('seq', 'head')
- grad_step: float32 [8192, 112], P('seq', 'head')
- grad_input_coeff: float32 [8192, 128], P('seq')
- grad_output_coeff: float32 [8192, 128], P('seq')
- grad_conv_weight: float32 [4, 7168], P(None, 'head')
- grad_step_bias: float32 [112], P('head')
- grad_rate_log: float32 [112], P('head')
- grad_skip: float32 [112], P('head')
The draws below stay inside these ranges and needn't reach their ends.
Inputs may be any that keep to these rules, and one draw needn't show every extreme that they name: doc_ids never fall along the sequence.
All inputs are finite; a program needn't handle non-finite values.
Results may differ from the reference program's by a relative error of at most 0.012.
Values may be sent and summed in bfloat16 or wider, within the bound.
A program may use at most 128 MiB of HBM per device.

```python
import math
import jax
import jax.numpy as jnp
import numpy as np
from jax import lax

T_DEV = 256
HEADS = 16
HEAD_DIM = 224
WINDOW = 1024
SSM_HEADS = 112
SSM_DIM = 64
STATE = 64
GROUPS = 2
KERNEL = 4
STRETCH = 128
SEQLEN = 8192
INNER = 7168
DOCS = 8


def aligned_pair(key):
    shape = (SEQLEN, HEADS * HEAD_DIM)
    normal_query = jax.random.truncated_normal(jax.random.fold_in(key, 11), -4.5, 4.5, shape, jnp.float32)
    normal_key = jax.random.truncated_normal(jax.random.fold_in(key, 12), -4.5, 4.5, shape, jnp.float32)
    return (normal_query, normal_key)


def draw_queries(key, part):
    return aligned_pair(key)[0].astype(jnp.bfloat16)


def draw_keys(key, part):
    return aligned_pair(key)[1].astype(jnp.bfloat16)


def draw_step_raw(key, part):
    blocks = SEQLEN // STRETCH
    offsets = jax.random.uniform(jax.random.fold_in(key, 21), (blocks, 1, SSM_HEADS), jnp.float32, -1.0, 1.0)
    noise = 0.5 * jax.random.truncated_normal(jax.random.fold_in(key, 23), -5.0, 5.0, (blocks, STRETCH, SSM_HEADS), jnp.float32)
    return (noise + offsets).reshape(SEQLEN, SSM_HEADS)


def draw_rate_log(key, part):
    chance = 0.5
    picked = jax.random.uniform(jax.random.fold_in(key, 31), (SSM_HEADS,), jnp.float32) < chance
    quick = jnp.log(jax.random.uniform(jax.random.fold_in(key, 32), (SSM_HEADS,), jnp.float32, 0.05, 0.3))
    slowly = jnp.log(jax.random.uniform(jax.random.fold_in(key, 33), (SSM_HEADS,), jnp.float32, 0.3, 2.0) / SEQLEN)
    return jnp.where(picked, quick, slowly)


def level_of(rng, shape, cuts, least, top_value):
    factor_of = 1.0
    for dim, shards_of in cuts:
        steps = jax.random.uniform(jax.random.fold_in(jax.random.fold_in(rng, 6), dim), (shards_of,), jnp.float32, least / len(cuts), top_value / len(cuts))
        factor_of = factor_of * jnp.repeat(jnp.exp(steps), shape[dim] // shards_of).reshape((-1,) + (1,) * (len(shape) - 1 - dim))
    return factor_of


def length_profile(count, total, bound, skew):
    loads = [(1 << 20) // math.isqrt(standing ** skew) + 1 for standing in range(2, count + 1)]
    rest, holding = total - bound - (count - 1), [1] * (count - 1)
    while rest > 0:
        free = [i for i in range(count - 1) if holding[i] < bound]
        whole, left = sum([loads[i] for i in free]), rest
        for i in free:
            addition = min(bound - holding[i], max(1, left * loads[i] // whole), rest)
            holding[i] = holding[i] + addition
            rest = rest - addition
    return np.array([bound] + holding)


def ragged_sizes(rng, number_of, total, reach, slope):
    if number_of == 2:
        one = jax.random.randint(rng, (), max(1, total - reach), min(reach, total - 1) + 1)
        return jnp.stack([one, total - one])
    sizes = jnp.asarray(length_profile(number_of, total, reach, slope), jnp.int32)
    twos = (number_of - 1) // 2
    giver, sink = sizes[1:1 + 2 * twos:2], sizes[2:2 + 2 * twos:2]
    margin = jnp.minimum(giver - 1, reach - sink)
    moved = jax.random.randint(jax.random.fold_in(rng, 1), (twos,), 0, 1 << 20) % (margin + 1)
    sizes = sizes.at[1:1 + 2 * twos:2].set(giver - moved).at[2:2 + 2 * twos:2].set(sink + moved)
    return sizes[jax.random.permutation(jax.random.fold_in(rng, 2), number_of)]


def bell_draw(key, shape, scale, most, split=(), kind=jnp.bfloat16):
    entries = jax.random.normal(key, shape, jnp.float32) * scale
    if len(split) > 0:
        entries = level_of(key, shape, split, -0.22, 0.18) * entries
    return jnp.clip(entries, min=-most, max=most).astype(kind)


def setup_inputs(seed: int = 0) -> dict:
    arg_keys = jax.random.split(jax.random.key(seed), 16)
    queries = draw_queries(jax.random.fold_in(arg_keys[15], 71), 0)
    keys = draw_keys(jax.random.fold_in(arg_keys[15], 71), 0)
    values = bell_draw(arg_keys[2], (SEQLEN, HEADS * HEAD_DIM), 1.0, 6.0, ((0, 32), (1, 4)))
    attn_grad = bell_draw(arg_keys[3], (SEQLEN, HEADS * HEAD_DIM), 1.0, 6.0, ((0, 32), (1, 4)))
    doc_ids = jnp.searchsorted(jnp.cumsum(ragged_sizes(arg_keys[4], DOCS, SEQLEN, SEQLEN // 2, 2)), jnp.arange(SEQLEN), side="right").astype(jnp.int32)
    conv_input = bell_draw(arg_keys[5], (SEQLEN, INNER), 1.0, 6.0, ((0, 32), (1, 4)))
    conv_weight = bell_draw(arg_keys[6], (KERNEL, INNER), KERNEL ** -0.5, 3.0, ((1, 4),), jnp.float32)
    step_raw = draw_step_raw(jax.random.fold_in(arg_keys[15], 71), 0)
    step_bias = jnp.clip(-1.5 + 1.5 * jax.random.uniform(arg_keys[8], (SSM_HEADS,), jnp.float32) ** level_of(arg_keys[8], (SSM_HEADS,), ((0, 4),), -0.2, 0.2), -1.5, 0.0)
    rate_log = draw_rate_log(jax.random.fold_in(arg_keys[15], 71), 0)
    skip_gain = jnp.clip(0.5 + 1.0 * jax.random.uniform(arg_keys[10], (SSM_HEADS,), jnp.float32) ** level_of(arg_keys[10], (SSM_HEADS,), ((0, 4),), -0.2, 0.2), 0.5, 1.5)
    input_coeff = bell_draw(arg_keys[11], (SEQLEN, GROUPS * STATE), 0.1, 0.625, ((0, 32),))
    output_coeff = bell_draw(arg_keys[12], (SEQLEN, GROUPS * STATE), 0.1, 0.625, ((0, 32),))
    gate_input = bell_draw(arg_keys[13], (SEQLEN, INNER), 1.0, 6.0, ((0, 32), (1, 4)))
    mix_grad = bell_draw(arg_keys[14], (SEQLEN, INNER), 0.25, 1.5, ((0, 32), (1, 4)))
    return dict(queries=queries, keys=keys, values=values, attn_grad=attn_grad, doc_ids=doc_ids, conv_input=conv_input, conv_weight=conv_weight, step_raw=step_raw, step_bias=step_bias, rate_log=rate_log, skip_gain=skip_gain, input_coeff=input_coeff, output_coeff=output_coeff, gate_input=gate_input, mix_grad=mix_grad)


NEG_FILL = -1e+30
EXACT = lax.Precision.HIGHEST

def conv_act(padded, doc_ext, weight):
    kernel_taps = weight.shape[0]
    length = padded.shape[0] - kernel_taps + 1
    doc_now = doc_ext[kernel_taps - 1:]
    summed = jnp.zeros((length, padded.shape[1]), jnp.float32)
    for lagged in range(kernel_taps):
        first_row = kernel_taps - 1 - lagged
        shifted = padded[first_row:first_row + length]
        same_doc = doc_ext[first_row:first_row + length] == doc_now
        summed = summed + weight[lagged] * jnp.where(same_doc[:, None], shifted, 0.0)
    return jax.nn.silu(summed)

def stretch_layout(log_decay, doc_row, doc_before):
    blocks = doc_row.shape[0] // STRETCH
    cumulative = jnp.cumsum(log_decay.reshape(blocks, STRETCH), axis=1)
    doc_grid = doc_row.reshape(blocks, STRETCH)
    previous = jnp.concatenate([jnp.reshape(doc_before, (1,)), doc_grid[:-1, -1]])
    return (cumulative, doc_grid, previous)

def head_final(head_act, step_size, log_decay, in_grid, start_state, doc_row, doc_before):
    cumulative, doc_grid, previous = stretch_layout(log_decay, doc_row, doc_before)
    blocks = cumulative.shape[0]
    scaled = (head_act * step_size[:, None]).reshape(blocks, STRETCH, head_act.shape[1])
    same_end = doc_grid == doc_grid[:, -1:]
    to_end = jnp.where(same_end, jnp.exp(jnp.where(same_end, cumulative[:, -1:] - cumulative, 0.0)), 0.0)
    local_state = jnp.einsum('cjp,cjn->cpn', scaled * to_end[:, :, None], in_grid, precision=EXACT)
    through = jnp.where(doc_grid[:, -1] == previous, jnp.exp(cumulative[:, -1]), 0.0)

    def advance(carry_state, pair_item):
        return (pair_item[0] * carry_state + pair_item[1], carry_state)
    final_state, starts = lax.scan(advance, start_state, (through, local_state))
    return (final_state, starts, cumulative, doc_grid, previous, scaled)

def head_output(head_act, step_size, log_decay, pair_grid, in_grid, out_grid, gate_part, skip_gain, start_state, doc_row, doc_before):
    final_state, starts, cumulative, doc_grid, previous, scaled = head_final(head_act, step_size, log_decay, in_grid, start_state, doc_row, doc_before)
    causal = jnp.arange(STRETCH)[:, None] >= jnp.arange(STRETCH)[None, :]
    same_doc = (doc_grid[:, :, None] == doc_grid[:, None, :]) & causal[None]
    weights = jnp.where(same_doc, jnp.exp(jnp.where(same_doc, cumulative[:, :, None] - cumulative[:, None, :], 0.0)), 0.0)
    inner_part = jnp.einsum('cij,cjp->cip', pair_grid * weights, scaled, precision=EXACT)
    enter_gain = jnp.where(doc_grid == previous[:, None], jnp.exp(cumulative), 0.0)
    carried = jnp.einsum('cin,cpn->cip', out_grid, starts, precision=EXACT) * enter_gain[:, :, None]
    mixed_out = (inner_part + carried).reshape(head_act.shape) + skip_gain * head_act
    return (mixed_out * jax.nn.silu(gate_part), final_state)

def round_edge(term):
    edge = lax.optimization_barrier(term[:WINDOW].astype(jnp.bfloat16)).astype(jnp.float32)
    return jnp.concatenate([edge, term[WINDOW:]], axis=0)

def attention_grads(queries, keys, values, attn_grad, doc_ids):
    width = HEADS * HEAD_DIM
    span = WINDOW + T_DEV
    scale = HEAD_DIM ** (-0.5)
    key_pad = jnp.concatenate([jnp.zeros((WINDOW, width), keys.dtype), keys])
    value_pad = jnp.concatenate([jnp.zeros((WINDOW, width), values.dtype), values])
    doc_pad = jnp.concatenate([jnp.full((WINDOW,), -1, jnp.int32), doc_ids])
    distance = jnp.arange(T_DEV)[:, None] + WINDOW - jnp.arange(span)[None, :]
    in_window = (distance >= 0) & (distance < WINDOW)

    def one_block(carry, index):
        key_acc, value_acc = carry
        first_row = index * T_DEV
        query_part = lax.dynamic_slice_in_dim(queries, first_row, T_DEV).astype(jnp.float32).reshape(T_DEV, HEADS, HEAD_DIM)
        grad_part = lax.dynamic_slice_in_dim(attn_grad, first_row, T_DEV).astype(jnp.float32).reshape(T_DEV, HEADS, HEAD_DIM)
        key_part = lax.dynamic_slice_in_dim(key_pad, first_row, span).astype(jnp.float32).reshape(span, HEADS, HEAD_DIM)
        value_part = lax.dynamic_slice_in_dim(value_pad, first_row, span).astype(jnp.float32).reshape(span, HEADS, HEAD_DIM)
        doc_query = lax.dynamic_slice_in_dim(doc_ids, first_row, T_DEV)
        doc_key = lax.dynamic_slice_in_dim(doc_pad, first_row, span)
        allowed = in_window & (doc_query[:, None] == doc_key[None, :])
        scores = jnp.where(allowed[None], jnp.einsum('ihd,jhd->hij', query_part, key_part) * scale, NEG_FILL)
        row_max = lax.optimization_barrier(jnp.max(scores, axis=-1))
        expo = jnp.where(allowed[None], jnp.exp(scores - row_max[:, :, None]), 0.0)
        row_sum = lax.optimization_barrier(jnp.sum(expo, axis=-1))
        probs = expo / jnp.maximum(row_sum, 1.0)[:, :, None]
        probs_half = lax.optimization_barrier(probs.astype(jnp.bfloat16)).astype(jnp.float32)
        attn_out = jnp.einsum('hij,jhd->ihd', probs_half, value_part)
        delta = lax.optimization_barrier(jnp.sum(grad_part * attn_out, axis=-1)).T
        dprob = jnp.einsum('ihd,jhd->hij', grad_part, value_part)
        dscore = lax.optimization_barrier((probs * (dprob - delta[:, :, None])).astype(jnp.bfloat16)).astype(jnp.float32)
        grad_query = (jnp.einsum('hij,jhd->ihd', dscore, key_part) * scale).reshape(T_DEV, width).astype(jnp.bfloat16)
        key_term = round_edge(jnp.einsum('hij,ihd->jhd', dscore, query_part).reshape(span, width))
        value_term = round_edge(jnp.einsum('hij,ihd->jhd', probs_half, grad_part).reshape(span, width))
        key_acc = lax.dynamic_update_slice_in_dim(key_acc, lax.dynamic_slice_in_dim(key_acc, first_row, span) + key_term, first_row, 0)
        value_acc = lax.dynamic_update_slice_in_dim(value_acc, lax.dynamic_slice_in_dim(value_acc, first_row, span) + value_term, first_row, 0)
        return ((key_acc, value_acc), grad_query)
    zero_acc = jnp.zeros((WINDOW + SEQLEN, width), jnp.float32)
    (key_acc, value_acc), grad_blocks = lax.scan(one_block, (zero_acc, zero_acc), jnp.arange(SEQLEN // T_DEV, dtype=jnp.int32))
    grad_queries = grad_blocks.reshape(SEQLEN, width)
    grad_keys = (key_acc[WINDOW:] * scale).astype(jnp.bfloat16)
    grad_values = value_acc[WINDOW:].astype(jnp.bfloat16)
    return (grad_queries, grad_keys, grad_values)

def mixer_grads(doc_ids, conv_input, conv_weight, step_raw, step_bias, rate_log, skip_gain, input_coeff, output_coeff, gate_input, mix_grad):
    doc_ext = jnp.concatenate([jnp.full((KERNEL - 1,), -1, jnp.int32), doc_ids])
    padded_all = jnp.concatenate([jnp.zeros((KERNEL - 1, INNER), jnp.float32), conv_input.astype(jnp.float32)])
    group_heads = SSM_HEADS // GROUPS
    blocks = SEQLEN // STRETCH
    zero_state = jnp.zeros((SSM_DIM, STATE), jnp.float32)
    start_doc = jnp.int32(-1)

    def forward(padded, weight, raw_step, bias_one, rate_one, skip_one, group_in, group_out, gate_part):
        head_act = conv_act(padded, doc_ext, weight)
        step_size = jax.nn.softplus(raw_step + bias_one)
        log_decay = -step_size * jnp.exp(rate_one)
        in_grid = group_in.reshape(blocks, STRETCH, STATE)
        out_grid = group_out.reshape(blocks, STRETCH, STATE)
        pair_grid = jnp.einsum('cin,cjn->cij', out_grid, in_grid, precision=EXACT)
        return head_output(head_act, step_size, log_decay, pair_grid, in_grid, out_grid, gate_part, skip_one, zero_state, doc_ids, start_doc)[0]

    def one_head(carry, head_index):
        sum_in, sum_out = carry
        column = head_index * SSM_DIM
        group_col = head_index // group_heads * STATE
        primals = (lax.dynamic_slice_in_dim(padded_all, column, SSM_DIM, 1), lax.dynamic_slice_in_dim(conv_weight, column, SSM_DIM, 1), lax.dynamic_index_in_dim(step_raw, head_index, 1, keepdims=False), step_bias[head_index], rate_log[head_index], skip_gain[head_index], lax.dynamic_slice_in_dim(input_coeff, group_col, STATE, 1).astype(jnp.float32), lax.dynamic_slice_in_dim(output_coeff, group_col, STATE, 1).astype(jnp.float32), lax.dynamic_slice_in_dim(gate_input, column, SSM_DIM, 1).astype(jnp.float32))
        cotangent = lax.dynamic_slice_in_dim(mix_grad, column, SSM_DIM, 1).astype(jnp.float32)
        gradients = jax.vjp(forward, *primals)[1](cotangent)
        sum_in = lax.dynamic_update_slice_in_dim(sum_in, lax.dynamic_slice_in_dim(sum_in, group_col, STATE, 1) + gradients[6], group_col, 1)
        sum_out = lax.dynamic_update_slice_in_dim(sum_out, lax.dynamic_slice_in_dim(sum_out, group_col, STATE, 1) + gradients[7], group_col, 1)
        return ((sum_in, sum_out), (gradients[0][KERNEL - 1:].astype(jnp.bfloat16), gradients[8].astype(jnp.bfloat16), gradients[2], gradients[1], gradients[3], gradients[4], gradients[5]))
    zero_cols = jnp.zeros((SEQLEN, GROUPS * STATE), jnp.float32)
    (sum_in, sum_out), stacked = lax.scan(one_head, (zero_cols, zero_cols), jnp.arange(SSM_HEADS, dtype=jnp.int32))
    conv_grad, gate_grad, step_grad, weight_grad, bias_grad, rate_grad, skip_grad = stacked
    grad_conv_input = jnp.transpose(conv_grad, (1, 0, 2)).reshape(SEQLEN, INNER)
    grad_gate = jnp.transpose(gate_grad, (1, 0, 2)).reshape(SEQLEN, INNER)
    grad_conv_weight = jnp.transpose(weight_grad, (1, 0, 2)).reshape(KERNEL, INNER)
    return (grad_conv_input, grad_gate, step_grad.T, sum_in, sum_out, grad_conv_weight, bias_grad, rate_grad, skip_grad)

def reference(queries, keys, values, attn_grad, doc_ids, conv_input, conv_weight, step_raw, step_bias, rate_log, skip_gain, input_coeff, output_coeff, gate_input, mix_grad):
    grad_queries, grad_keys, grad_values = attention_grads(queries, keys, values, attn_grad, doc_ids)
    grad_conv_input, grad_gate, grad_step, grad_input_coeff, grad_output_coeff, grad_conv_weight, grad_step_bias, grad_rate_log, grad_skip = mixer_grads(doc_ids, conv_input, conv_weight, step_raw, step_bias, rate_log, skip_gain, input_coeff, output_coeff, gate_input, mix_grad)
    return (grad_queries, grad_keys, grad_values, grad_conv_input, grad_gate, grad_step, grad_input_coeff, grad_output_coeff, grad_conv_weight, grad_step_bias, grad_rate_log, grad_skip)
```

```python
import functools

import jax
import jax.numpy as jnp
from jax import lax
from jax.experimental import pallas as pl
from jax.experimental.pallas import tpu as pltpu
from jax.sharding import PartitionSpec as P

HEAD_DIM = 224
WINDOW = 1024
SSM_HEADS = 112
STATE = 64
GROUPS = 2
T = 256
NH = 28
PAIRS = 14
NSEQ = 32
RING = 4
NEG = -1e30
F32 = jnp.float32
BF16 = jnp.bfloat16
MESH = pl.DeviceIdType.MESH
VM = pltpu.VMEM
SCALE = HEAD_DIM ** (-0.5)
HI = lax.Precision.HIGHEST


def dot(a, b, ca, cb, precision=None):
    return lax.dot_general(
        a, b, (((ca,), (cb,)), ((), ())), preferred_element_type=F32, precision=precision
    )


def sigmoid(v):
    return 1.0 / (1.0 + jnp.exp(-v))


def col_of(row, rows):
    return jnp.transpose(jnp.broadcast_to(row, (rows, row.shape[1])))


def prep_kernel(q_ref, k_ref, v_ref, g_ref, *refs):
    kv, qd, scr = refs[:4], refs[4:8], refs[8]
    x = lax.rem(lax.axis_index("seq"), RING)
    for slot, (src, dest) in enumerate(((k_ref, kv), (v_ref, kv), (q_ref, qd), (g_ref, qd))):
        scr[...] = jnp.transpose(src[...].astype(F32)).astype(BF16)
        for k in range(RING):
            h = lax.rem(x + k, RING)
            dest[k][slot % 2] = scr[pl.ds(pl.multiple_of(h * HEAD_DIM, 32), HEAD_DIM), :]


def attn_prep(queries, keys, values, attn_grad):
    piece = jax.ShapeDtypeStruct((2, HEAD_DIM, T), BF16)
    return pl.pallas_call(
        prep_kernel,
        out_shape=[piece] * 8,
        scratch_shapes=[VM((4 * HEAD_DIM, T), BF16)],
        name="attn_prep",
        cost_estimate=pl.CostEstimate(flops=4000000, bytes_accessed=4000000, transcendentals=0),
    )(queries, keys, values, attn_grad)


def attn_kernel(*refs):
    kv, qd, halo, doc_ref = refs[0:4], refs[4:8], refs[8:12], refs[12]
    own, back = refs[13:17], refs[17:21]
    akv, aqd, dka, dva, doq = refs[21:26]
    x = lax.rem(lax.axis_index("seq"), RING)
    for k in range(RING):
        c = lax.rem(x - k + RING, RING)
        akv[RING + c] = kv[k][...]
        akv[c] = halo[k][...]
        aqd[c] = qd[k][...]
    dka[...] = jnp.zeros_like(dka)
    dva[...] = jnp.zeros_like(dva)
    row_i = lax.broadcasted_iota(jnp.int32, (T, T), 0)
    col_j = lax.broadcasted_iota(jnp.int32, (T, T), 1)

    def chunk(c, carry):
        qt = aqd[c, 0]
        gt = aqd[c, 1]
        q = jnp.transpose(qt.astype(F32)).astype(BF16)
        g = jnp.transpose(gt.astype(F32)).astype(BF16)
        dq_col = col_of(doc_ref[pl.ds(RING + c, 1), :], 128)
        dq_col = jnp.concatenate([dq_col, dq_col], axis=1)
        scores, masks = [], []
        row_max = None
        for b in range(RING + 1):
            s = dot(q, akv[c + b, 0], 1, 0) * SCALE
            ok = dq_col == doc_ref[pl.ds(c + b, 1), :]
            if b == 0:
                ok = ok & (col_j > row_i)
            if b == RING:
                ok = ok & (col_j <= row_i)
            s = jnp.where(ok, s, NEG)
            scores.append(s)
            masks.append(ok)
            m = jnp.max(s, axis=1, keepdims=True)
            row_max = m if row_max is None else jnp.maximum(row_max, m)
        row_sum = None
        for b in range(RING + 1):
            e = jnp.where(masks[b], jnp.exp(scores[b] - row_max), 0.0)
            scores[b] = e
            r = jnp.sum(e, axis=1, keepdims=True)
            row_sum = r if row_sum is None else row_sum + r
        inv = 1.0 / jnp.maximum(row_sum, 1.0)
        dprobs = []
        delta = None
        for b in range(RING + 1):
            p = scores[b] * inv
            scores[b] = p
            half = p.astype(BF16)
            dp = dot(g, akv[c + b, 1], 1, 0)
            dprobs.append(dp)
            r = jnp.sum(half.astype(F32) * dp, axis=1, keepdims=True)
            delta = r if delta is None else delta + r
            dva[c + b] = dva[c + b] + dot(gt, half, 1, 0)
        dqt = None
        for b in range(RING + 1):
            ds = (scores[b] * (dprobs[b] - delta)).astype(BF16)
            r = dot(akv[c + b, 0], ds, 1, 1)
            dqt = r if dqt is None else dqt + r
            dka[c + b] = dka[c + b] + dot(qt, ds, 1, 0)
        doq[c] = dqt
        return carry

    lax.fori_loop(0, RING, chunk, 0)
    for k in range(RING):
        c = lax.rem(x + k, RING)
        own[k][0] = (doq[c] * SCALE).astype(BF16)
        own[k][1] = (dka[RING + c] * SCALE).astype(BF16)
        own[k][2] = dva[RING + c].astype(BF16)
        back[k][0] = (dka[c] * SCALE).astype(BF16)
        back[k][1] = dva[c].astype(BF16)


def attn_core(kv, qd, halo, doc_rows):
    return pl.pallas_call(
        attn_kernel,
        out_shape=[jax.ShapeDtypeStruct((3, HEAD_DIM, T), BF16)] * 4
        + [jax.ShapeDtypeStruct((2, HEAD_DIM, T), BF16)] * 4,
        scratch_shapes=[
            VM((2 * RING, 2, HEAD_DIM, T), BF16),
            VM((RING, 2, HEAD_DIM, T), BF16),
            VM((2 * RING, HEAD_DIM, T), F32),
            VM((2 * RING, HEAD_DIM, T), F32),
            VM((RING, HEAD_DIM, T), F32),
        ],
        name="attn_core",
        cost_estimate=pl.CostEstimate(
            flops=3000000000, bytes_accessed=8000000, transcendentals=1400000
        ),
    )(*kv, *qd, *halo, doc_rows)


def attn_final_kernel(*refs):
    own, back = refs[0:4], refs[4:8]
    dq_ref, dk_ref, dv_ref, scr = refs[8:12]
    x = lax.rem(lax.axis_index("seq"), RING)
    for slot, dest in enumerate((dq_ref, dk_ref, dv_ref)):
        for k in range(RING):
            h = lax.rem(x - k + RING, RING)
            part = own[k][slot].astype(F32)
            if slot:
                part = part + back[k][slot - 1].astype(F32)
            scr[pl.ds(pl.multiple_of(h * HEAD_DIM, 32), HEAD_DIM), :] = part
        dest[...] = jnp.transpose(scr[...]).astype(BF16)


def attn_final(own, back):
    whole = jax.ShapeDtypeStruct((T, 4 * HEAD_DIM), BF16)
    return pl.pallas_call(
        attn_final_kernel,
        out_shape=[whole] * 3,
        scratch_shapes=[VM((4 * HEAD_DIM, T), F32)],
        name="attn_final",
        cost_estimate=pl.CostEstimate(flops=4000000, bytes_accessed=4000000, transcendentals=0),
    )(*own, *back)


def ring_shift(value, k):
    if k == 0:
        return value
    return lax.ppermute(
        value, "seq", [(s, s // RING * RING + (s + k) % RING) for s in range(NSEQ)]
    )


def group_shift(value, k, step):
    pairs = []
    for s in range(NSEQ):
        group, x = divmod(s, RING)
        if 0 <= group + step < NSEQ // RING:
            pairs.append((s, (group + step) * RING + (x + k) % RING))
    return lax.ppermute(value, "seq", pairs)


def mixer_setup(raw_ref, bias_ref, rate_ref, docc_ref, rows, tri, scr, mk):
    scr[...] = jnp.zeros_like(scr)
    step = jnp.log(1.0 + jnp.exp(raw_ref[...] + bias_ref[...]))
    scr[:, 0:NH] = step
    rows[0] = jnp.transpose(scr[...])[0:32]
    scr[:, 0:NH] = -step * jnp.exp(rate_ref[...])
    ld = jnp.transpose(scr[...])[0:32]
    rows[1] = ld
    i = lax.broadcasted_iota(jnp.int32, (T, T), 0)
    j = lax.broadcasted_iota(jnp.int32, (T, T), 1)
    tri[...] = jnp.where(i <= j, 1.0, 0.0)
    cum = dot(ld, tri[...], 1, 0, HI)
    rows[2] = cum
    rows[3] = jnp.where(docc_ref[1:2, :] > 0.0, jnp.exp(cum), 0.0)
    rows[4] = jnp.where(
        docc_ref[2:3, :] > 0.0, jnp.exp(jnp.minimum(cum[:, T - 1 : T] - cum, 0.0)), 0.0
    )
    for k in range(3):
        mk[k] = col_of(docc_ref[3 + k : 4 + k, :], 128)


def pair_rows(rows, which, pair):
    a = rows[which, pl.ds(2 * pair, 1), :]
    b = rows[which, pl.ds(2 * pair + 1, 1), :]
    return jnp.concatenate(
        [jnp.broadcast_to(a, (64, T)), jnp.broadcast_to(b, (64, T))], axis=0
    )


def group_cols(ref, group):
    v = ref[...].astype(F32)
    return jnp.where(group == 0, v[:, 0:STATE], v[:, STATE:])


def conv_forward(x, tail_ref, w_ref, mk, xs):
    xs[0:8, :] = tail_ref[...]
    xs[8 : 8 + T, :] = x
    pre = w_ref[0:1, :] * x
    for k in range(1, 4):
        pre = pre + w_ref[k : k + 1, :] * (mk[k - 1] * xs[8 - k : 8 - k + T, :])
    return pre


def phase_a_kernel(
    conv_ref, tail_ref, gate_ref, mix_ref, w_ref, raw_ref, bias_ref, rate_ref, docc_ref,
    bin_ref, cout_ref,
    act_out, g_out, loc_out, thr_out,
    rows, tri, scr, mk, xs, bg, cg,
):
    pair = pl.program_id(0)

    @pl.when(pair == 0)
    def _():
        mixer_setup(raw_ref, bias_ref, rate_ref, docc_ref, rows, tri, scr, mk)
        group = lax.axis_index("head") // 2
        bg[...] = group_cols(bin_ref, group).astype(BF16)
        cg[...] = group_cols(cout_ref, group).astype(BF16)
        thr = rows[3][:, T - 1 : T]
        thr_out[...] = jnp.broadcast_to(thr, (32, 128))

    x = conv_ref[...].astype(F32)
    pre = conv_forward(x, tail_ref, w_ref, mk, xs)
    act = pre * sigmoid(pre)
    gate = gate_ref[...].astype(F32)
    g = mix_ref[...].astype(F32) * (gate * sigmoid(gate))
    act_t = jnp.transpose(act)
    g_t = jnp.transpose(g)
    act_out[...] = act_t
    g_out[...] = g_t
    st = act_t * (pair_rows(rows, 0, pair) * pair_rows(rows, 4, pair))
    ge = g_t * pair_rows(rows, 3, pair)
    loc_out[:, 0:STATE] = dot(st.astype(BF16), bg[...], 1, 0).astype(BF16)
    loc_out[:, STATE:] = dot(ge.astype(BF16), cg[...], 1, 0).astype(BF16)


def whole_spec(shape):
    return pl.BlockSpec(shape, lambda i: (0,) * len(shape))


def phase_a(conv_input, tail8, gate_input, mix_grad, conv_weight, raw, bias, rate, docc, bin_, cout):
    tok = pl.BlockSpec((T, 128), lambda i: (0, i))
    chan = pl.BlockSpec((128, T), lambda i: (i, 0))
    return pl.pallas_call(
        phase_a_kernel,
        grid=(PAIRS,),
        in_specs=[
            tok,
            pl.BlockSpec((8, 128), lambda i: (0, i)),
            tok,
            tok,
            pl.BlockSpec((4, 128), lambda i: (0, i)),
            whole_spec((T, NH)),
            whole_spec((1, NH)),
            whole_spec((1, NH)),
            whole_spec((8, T)),
            whole_spec((T, 128)),
            whole_spec((T, 128)),
        ],
        out_specs=[
            chan,
            chan,
            pl.BlockSpec((128, 128), lambda i: (i, 0)),
            whole_spec((32, 128)),
        ],
        out_shape=[
            jax.ShapeDtypeStruct((NH * 64, T), F32),
            jax.ShapeDtypeStruct((NH * 64, T), F32),
            jax.ShapeDtypeStruct((NH * 64, 128), BF16),
            jax.ShapeDtypeStruct((32, 128), F32),
        ],
        scratch_shapes=[
            VM((5, 32, T), F32),
            VM((T, T), F32),
            VM((T, 128), F32),
            VM((3, T, 128), F32),
            VM((8 + T, 128), F32),
            VM((T, STATE), BF16),
            VM((T, STATE), BF16),
        ],
        name="mixer_a",
        cost_estimate=pl.CostEstimate(
            flops=600000000, bytes_accessed=7000000, transcendentals=1000000
        ),
    )(conv_input, tail8, gate_input, mix_grad, conv_weight, raw, bias, rate, docc, bin_, cout)


def phase_b_kernel(
    conv_ref, tail_ref, gate_ref, mix_ref, w_ref, raw_ref, bias_ref, rate_ref, docc_ref,
    bin_ref, cout_ref, act_ref, g_ref, st_ref, skip_ref,
    dconv_out, dgate_out, spill_out, last_out, red_out, step_out, scal_out, coef_out,
    rows, tri, scr, mk, xs, bg, cg, cgt, bias_m, pair_t, dpair, dcum, ddir, dskp, dbt, dct, qs,
):
    pair = pl.program_id(0)

    @pl.when(pair == 0)
    def _():
        mixer_setup(raw_ref, bias_ref, rate_ref, docc_ref, rows, tri, scr, mk)
        group = lax.axis_index("head") // 2
        bf = group_cols(bin_ref, group)
        cf = group_cols(cout_ref, group)
        bg[...] = bf.astype(BF16)
        cg[...] = cf.astype(BF16)
        pair_t[...] = dot(bf, cf, 1, 1, HI)
        doc = docc_ref[0:1, :]
        dcol = col_of(doc, 128)
        dcol = jnp.concatenate([dcol, dcol], axis=1)
        ok = (tri[...] > 0.5) & (dcol == doc)
        bias_m[...] = jnp.where(ok, 0.0, NEG)
        dpair[...] = jnp.zeros_like(dpair)
        dbt[...] = jnp.zeros_like(dbt)
        dct[...] = jnp.zeros_like(dct)
        dcum[...] = jnp.zeros_like(dcum)
        ddir[...] = jnp.zeros_like(ddir)
        dskp[...] = jnp.zeros_like(dskp)
        qs[...] = jnp.zeros_like(qs)
        scal_out[...] = jnp.zeros_like(scal_out)

    act_t = act_ref[...]
    g_t = g_ref[...]
    step_p = pair_rows(rows, 0, pair)
    eg_p = pair_rows(rows, 3, pair)
    te_p = pair_rows(rows, 4, pair)
    s_t = act_t * step_p
    s_b = s_t.astype(BF16)
    g_b = g_t.astype(BF16)
    state = st_ref[...]
    start = state[:, 0:STATE]
    end = state[:, STATE:]
    car = dot(start, cg[...], 1, 1) * eg_p
    dste = dot(end, bg[...], 1, 1) * te_p
    dct[...] += dot(start, (g_t * eg_p).astype(BF16), 0, 0)
    dbt[...] += dot(end, (s_t * te_p).astype(BF16), 0, 0)
    se = start.astype(F32) * end.astype(F32)
    lane = lax.broadcasted_iota(jnp.int32, (1, T), 1)
    ys, dss = [], []
    for a in range(2):
        lo = 64 * a
        h = 2 * pair + a
        cum = rows[2, pl.ds(h, 1), :]
        cc = col_of(cum, 128)
        cc = jnp.concatenate([cc, cc], axis=1)
        w = jnp.exp(jnp.minimum(cum - cc, 0.0) + bias_m[...])
        m = pair_t[...] * w
        mb = m.astype(BF16)
        sh = s_b[lo : lo + 64]
        gh = g_b[lo : lo + 64]
        y = dot(sh, mb, 1, 0)
        dsi = dot(gh, mb, 1, 1)
        dm = dot(sh, gh, 0, 0)
        dpair[...] += dm * w
        z = dm * m
        zr = jnp.sum(jnp.transpose(z[:, 0:128] + z[:, 128:]), axis=0, keepdims=True)
        carh = car[lo : lo + 64]
        dsth = dste[lo : lo + 64]
        gt = g_t[lo : lo + 64]
        st = s_t[lo : lo + 64]
        at = act_t[lo : lo + 64]
        v = jnp.sum(st * dsth, axis=0, keepdims=True)
        d = jnp.sum(z, axis=0, keepdims=True) - zr + jnp.sum(gt * carh, axis=0, keepdims=True) - v
        thr = rows[3, pl.ds(h, 1), :][:, T - 1 : T]
        extra = jnp.sum(v, axis=1, keepdims=True) + thr * jnp.sum(
            jnp.sum(se[lo : lo + 64], axis=0, keepdims=True), axis=1, keepdims=True
        )
        dcum[pl.ds(h, 1), :] = d + jnp.where(lane == T - 1, extra, 0.0)
        ds = dsi + dsth
        ddir[pl.ds(h, 1), :] = jnp.sum(ds * at, axis=0, keepdims=True)
        dskp[pl.ds(h, 1), :] = jnp.sum(gt * at, axis=0, keepdims=True)
        skip = skip_ref[h]
        ys.append(y + carh + skip * at)
        dss.append(ds * step_p[lo : lo + 64] + skip * gt)
    y = jnp.transpose(jnp.concatenate(ys, axis=0))
    dact = jnp.transpose(jnp.concatenate(dss, axis=0))
    gate = gate_ref[...].astype(F32)
    sg = sigmoid(gate)
    dgate_out[...] = (
        mix_ref[...].astype(F32) * y * (sg * (1.0 + gate * (1.0 - sg)))
    ).astype(BF16)
    x = conv_ref[...].astype(F32)
    pre = conv_forward(x, tail_ref, w_ref, mk, xs)
    sp = sigmoid(pre)
    dpre = dact * (sp * (1.0 + pre * (1.0 - sp)))
    dx = None
    for k in range(4):
        q = dpre if k == 0 else dpre * mk[k - 1]
        red_out[0, k : k + 1, :] = jnp.sum(q * xs[8 - k : 8 - k + T, :], axis=0, keepdims=True)
        qs[8 : 8 + T, :] = q
        term = w_ref[k : k + 1, :] * qs[k : k + 8 + T, :]
        dx = term if dx is None else dx + term
    spill_out[...] = dx[0:8]
    dconv_out[...] = dx[8:].astype(BF16)
    last_out[...] = dx[T:]
    red_out[0, 4:8, :] = jnp.zeros((4, 128), F32)

    @pl.when(pair == PAIRS - 1)
    def _():
        dld = dot(dcum[...], tri[...], 1, 1, HI)
        zero = jnp.zeros((96, T), F32)
        to_tok = lambda v: jnp.transpose(jnp.concatenate([v, zero], axis=0))[:, 0:NH]
        dld_t = to_tok(dld)
        dir_t = to_tok(ddir[...])
        rate = jnp.exp(rate_ref[...])
        v = raw_ref[...] + bias_ref[...]
        step = jnp.log(1.0 + jnp.exp(v))
        gs = (dir_t - dld_t * rate) * sigmoid(v)
        step_out[...] = gs
        scal_out[0:1, 0:NH] = jnp.sum(gs, axis=0, keepdims=True)
        scal_out[1:2, 0:NH] = -rate * jnp.sum(dld_t * step, axis=0, keepdims=True)
        scal_out[2:3, 0:NH] = jnp.sum(to_tok(dskp[...]), axis=0, keepdims=True)
        dp = dpair[...].astype(BF16)
        coef_out[0:STATE] = (dbt[...] + dot(jnp.transpose(cg[...].astype(F32)).astype(BF16), dp, 1, 1)).astype(BF16)
        coef_out[STATE:] = (dct[...] + dot(jnp.transpose(bg[...].astype(F32)).astype(BF16), dp, 1, 0)).astype(BF16)


def phase_b(
    conv_input, tail8, gate_input, mix_grad, conv_weight, raw, bias, rate, docc, bin_, cout,
    act_t, g_t, states, skip,
):
    tok = pl.BlockSpec((T, 128), lambda i: (0, i))
    chan = pl.BlockSpec((128, T), lambda i: (i, 0))
    row8 = pl.BlockSpec((8, 128), lambda i: (0, i))
    width = NH * 64
    return pl.pallas_call(
        phase_b_kernel,
        grid=(PAIRS,),
        in_specs=[
            tok,
            row8,
            tok,
            tok,
            pl.BlockSpec((4, 128), lambda i: (0, i)),
            whole_spec((T, NH)),
            whole_spec((1, NH)),
            whole_spec((1, NH)),
            whole_spec((8, T)),
            whole_spec((T, 128)),
            whole_spec((T, 128)),
            chan,
            chan,
            pl.BlockSpec((128, 128), lambda i: (i, 0)),
            pl.BlockSpec(memory_space=pltpu.SMEM),
        ],
        out_specs=[
            tok,
            tok,
            row8,
            row8,
            pl.BlockSpec((1, 8, 128), lambda i: (i, 0, 0)),
            whole_spec((T, NH)),
            whole_spec((8, 128)),
            whole_spec((128, T)),
        ],
        out_shape=[
            jax.ShapeDtypeStruct((T, width), BF16),
            jax.ShapeDtypeStruct((T, width), BF16),
            jax.ShapeDtypeStruct((8, width), F32),
            jax.ShapeDtypeStruct((8, width), F32),
            jax.ShapeDtypeStruct((PAIRS, 8, 128), F32),
            jax.ShapeDtypeStruct((T, NH), F32),
            jax.ShapeDtypeStruct((8, 128), F32),
            jax.ShapeDtypeStruct((128, T), BF16),
        ],
        scratch_shapes=[
            VM((5, 32, T), F32),
            VM((T, T), F32),
            VM((T, 128), F32),
            VM((3, T, 128), F32),
            VM((8 + T, 128), F32),
            VM((T, STATE), BF16),
            VM((T, STATE), BF16),
            VM((STATE, T), BF16),
            VM((T, T), F32),
            VM((T, T), F32),
            VM((T, T), F32),
            VM((32, T), F32),
            VM((32, T), F32),
            VM((32, T), F32),
            VM((STATE, T), F32),
            VM((STATE, T), F32),
            VM((16 + T, 128), F32),
        ],
        name="mixer_b",
        cost_estimate=pl.CostEstimate(
            flops=3000000000, bytes_accessed=10000000, transcendentals=3000000
        ),
    )(
        conv_input, tail8, gate_input, mix_grad, conv_weight, raw, bias, rate, docc, bin_, cout,
        act_t, g_t, states, skip,
    )


def seq_barrier(me):
    barrier = pltpu.get_barrier_semaphore()

    def greet(k, carry):
        peer = lax.rem(me + k, NSEQ)
        pl.semaphore_signal(barrier, inc=1, device_id={"seq": peer}, device_id_type=MESH)
        return carry

    lax.fori_loop(1, NSEQ, greet, 0)
    pl.semaphore_wait(barrier, NSEQ - 1)


def chain_kernel(loc_ref, thr_ref, out_ref, pay, inbox, outb, landed, s1, r1, s2, r2):
    me = lax.axis_index("seq")
    for e in range(NH):
        pay[e, 0:64, :] = loc_ref[e]
        t = thr_ref[e : e + 1, :]
        hi = t.astype(BF16)
        lo = (t - hi.astype(F32)).astype(BF16)
        pay[e, 64:80, :] = jnp.concatenate(
            [jnp.broadcast_to(hi, (8, 128)), jnp.broadcast_to(lo, (8, 128))], axis=0
        )
    seq_barrier(me)

    def first(peer, src):
        return pltpu.make_async_remote_copy(
            src_ref=pay.at[peer],
            dst_ref=inbox.at[src],
            send_sem=s1.at[peer],
            recv_sem=r1.at[src],
            device_id={"seq": peer},
            device_id_type=MESH,
        )

    def second(peer, src):
        return pltpu.make_async_remote_copy(
            src_ref=outb.at[peer],
            dst_ref=landed.at[src],
            send_sem=s2.at[peer],
            recv_sem=r2.at[src],
            device_id={"seq": peer},
            device_id_type=MESH,
        )

    def send_first(k, carry):
        peer = lax.rem(me + k, NSEQ)

        @pl.when(peer < NH)
        def _():
            first(peer, me).start()

        return carry

    lax.fori_loop(1, NSEQ, send_first, 0)

    @pl.when(me < NH)
    def _():
        inbox[me] = pay[me]

        def wait_first(k, carry):
            src = lax.rem(me + k, NSEQ)
            first(me, src).wait_recv()
            return carry

        lax.fori_loop(1, NSEQ, wait_first, 0)
        lane = lax.broadcasted_iota(jnp.int32, (64, 128), 1)

        def gain(s):
            return inbox[s, 64:65, :].astype(F32) + inbox[s, 72:73, :].astype(F32)

        def down(s, run):
            outb[s] = run.astype(BF16)
            return gain(s) * run + inbox[s, 0:64, :].astype(F32)

        lax.fori_loop(0, NSEQ, down, jnp.zeros((64, 128), F32))

        def up(k, run):
            s = NSEQ - 1 - k
            outb[s] = jnp.where(lane < STATE, outb[s], run.astype(BF16))
            return gain(s) * run + inbox[s, 0:64, :].astype(F32)

        lax.fori_loop(0, NSEQ, up, jnp.zeros((64, 128), F32))

        def send_second(k, carry):
            second(lax.rem(me + k, NSEQ), me).start()
            return carry

        lax.fori_loop(1, NSEQ, send_second, 0)
        landed[me] = outb[me]

    def finish(k, carry):
        peer = lax.rem(me + k, NSEQ)

        @pl.when(peer < NH)
        def _():
            first(peer, me).wait_send()
            second(me, peer).wait_recv()

        return carry

    lax.fori_loop(1, NSEQ, finish, 0)

    @pl.when(me < NH)
    def _():
        def drain(k, carry):
            second(lax.rem(me + k, NSEQ), me).wait_send()
            return carry

        lax.fori_loop(1, NSEQ, drain, 0)

    out_ref[...] = landed[...]


def chain(loc, thr):
    dma = pltpu.SemaphoreType.DMA
    return pl.pallas_call(
        chain_kernel,
        out_shape=jax.ShapeDtypeStruct((NH, 64, 128), BF16),
        scratch_shapes=[
            VM((NH, 80, 128), BF16),
            VM((NSEQ, 80, 128), BF16),
            VM((NSEQ, 64, 128), BF16),
            VM((NH, 64, 128), BF16),
            dma((NSEQ,)),
            dma((NSEQ,)),
            dma((NSEQ,)),
            dma((NSEQ,)),
        ],
        compiler_params=pltpu.CompilerParams(collective_id=1, has_side_effects=True),
        name="state_chain",
        cost_estimate=pl.CostEstimate(flops=20000000, bytes_accessed=1000000, transcendentals=0),
    )(loc, thr)


BLOCKS = PAIRS + 1


def sums_kernel(
    red_ref, scal_ref, coef_ref, spill_ref, last_ref,
    dw_ref, sc_ref, gin_ref, gout_ref, fix_ref,
    src, inbox, tot, cin, spin, s1, r1, s2, r2, s3, r3, s4, r4,
):
    me = lax.axis_index("seq")
    hd = lax.axis_index("head")
    barrier = pltpu.get_barrier_semaphore()

    def greet(k, carry):
        peer = lax.rem(me + k, NSEQ)
        pl.semaphore_signal(barrier, inc=1, device_id={"seq": peer}, device_id_type=MESH)
        return carry

    lax.fori_loop(1, NSEQ, greet, 0)
    for k in range(1, 4):
        pl.semaphore_signal(
            barrier, inc=1, device_id={"head": lax.rem(hd + k, 4)}, device_id_type=MESH
        )
    src[0:PAIRS] = red_ref[...]
    src[PAIRS] = scal_ref[...]
    pl.semaphore_wait(barrier, NSEQ + 2)

    def coef(k, frm):
        return pltpu.make_async_remote_copy(
            src_ref=coef_ref,
            dst_ref=cin.at[frm],
            send_sem=s3.at[k],
            recv_sem=r3.at[frm],
            device_id={"head": lax.rem(hd + k, 4)},
            device_id_type=MESH,
        )

    spill_copy = pltpu.make_async_remote_copy(
        src_ref=spill_ref,
        dst_ref=spin,
        send_sem=s4,
        recv_sem=r4,
        device_id={"seq": lax.rem(me + NSEQ - 1, NSEQ)},
        device_id_type=MESH,
    )

    def first(block, frm):
        return pltpu.make_async_remote_copy(
            src_ref=src.at[block],
            dst_ref=inbox.at[frm],
            send_sem=s1.at[block],
            recv_sem=r1.at[frm],
            device_id={"seq": 2 * block},
            device_id_type=MESH,
        )

    def second(peer, block):
        return pltpu.make_async_remote_copy(
            src_ref=tot.at[block],
            dst_ref=tot.at[block],
            send_sem=s2.at[peer],
            recv_sem=r2.at[block],
            device_id={"seq": peer},
            device_id_type=MESH,
        )

    def send_first(b, carry):
        @pl.when(2 * b != me)
        def _():
            first(b, me).start()

        return carry

    lax.fori_loop(0, BLOCKS, send_first, 0)
    for k in range(1, 4):
        coef(k, hd).start()
    spill_copy.start()
    mine = me // 2
    owner = (me == 2 * mine) & (mine < BLOCKS)

    @pl.when(owner)
    def _():
        inbox[me] = src[mine]

        def wait_first(k, carry):
            first(mine, lax.rem(me + k, NSEQ)).wait_recv()
            return carry

        lax.fori_loop(1, NSEQ, wait_first, 0)
        tot[mine] = jnp.sum(inbox[...], axis=0)

        def send_second(k, carry):
            second(lax.rem(me + k, NSEQ), mine).start()
            return carry

        lax.fori_loop(1, NSEQ, send_second, 0)

    for k in range(1, 4):
        coef(k, lax.rem(hd + k, 4)).wait_recv()
    cin[hd] = coef_ref[...]
    g0 = jnp.transpose(cin[0].astype(F32) + cin[1].astype(F32))
    g1 = jnp.transpose(cin[2].astype(F32) + cin[3].astype(F32))
    gin_ref[...] = jnp.concatenate([g0[:, 0:STATE], g1[:, 0:STATE]], axis=1)
    gout_ref[...] = jnp.concatenate([g0[:, STATE:], g1[:, STATE:]], axis=1)
    spill_copy.wait_recv()
    keep = jnp.where(me == NSEQ - 1, 0.0, 1.0)
    fix_ref[...] = last_ref[...] + keep * spin[...]

    def wait_second(b, carry):
        @pl.when(2 * b != me)
        def _():
            second(me, b).wait_recv()
            first(b, me).wait_send()

        return carry

    lax.fori_loop(0, BLOCKS, wait_second, 0)
    for p in range(PAIRS):
        dw_ref[:, 128 * p : 128 * p + 128] = tot[p, 0:4, :]
    sc_ref[...] = tot[PAIRS]

    @pl.when(owner)
    def _():
        def drain(k, carry):
            second(lax.rem(me + k, NSEQ), mine).wait_send()
            return carry

        lax.fori_loop(1, NSEQ, drain, 0)

    for k in range(1, 4):
        coef(k, hd).wait_send()
    spill_copy.wait_send()


def sums(red, scal, coef, spill, last):
    dma = pltpu.SemaphoreType.DMA
    width = NH * 64
    return pl.pallas_call(
        sums_kernel,
        out_shape=[
            jax.ShapeDtypeStruct((4, width), F32),
            jax.ShapeDtypeStruct((8, 128), F32),
            jax.ShapeDtypeStruct((T, 128), F32),
            jax.ShapeDtypeStruct((T, 128), F32),
            jax.ShapeDtypeStruct((8, width), F32),
        ],
        in_specs=[pl.BlockSpec(memory_space=VM)] * 5,
        out_specs=[pl.BlockSpec(memory_space=VM)] * 5,
        scratch_shapes=[
            VM((BLOCKS, 8, 128), F32),
            VM((NSEQ, 8, 128), F32),
            VM((BLOCKS, 8, 128), F32),
            VM((4, 128, T), BF16),
            VM((8, width), F32),
            dma((BLOCKS,)),
            dma((NSEQ,)),
            dma((NSEQ,)),
            dma((BLOCKS,)),
            dma((4,)),
            dma((4,)),
            dma,
            dma,
        ],
        compiler_params=pltpu.CompilerParams(collective_id=2, has_side_effects=True),
        name="sums",
        cost_estimate=pl.CostEstimate(flops=2000000, bytes_accessed=1000000, transcendentals=0),
    )(red, scal, coef, spill, last)


def local(
    queries, keys, values, attn_grad, doc_ids, conv_input, conv_weight, step_raw, step_bias,
    rate_log, skip_gain, input_coeff, output_coeff, gate_input, mix_grad,
):
    me = lax.axis_index("seq")
    pieces = attn_prep(queries, keys, values, attn_grad)
    halo = [group_shift(pieces[k], k, 1) for k in range(RING)]
    kv = [ring_shift(pieces[k], k) for k in range(RING)]
    qd = [ring_shift(pieces[4 + k], k) for k in range(RING)]
    tail = lax.ppermute(
        conv_input[T - 8 :], "seq", [(s, s + 1) for s in range(NSEQ - 1)]
    ).astype(F32)
    doc_pad = jnp.concatenate([jnp.full((WINDOW,), -1, jnp.int32), doc_ids])
    doc_rows = lax.dynamic_slice_in_dim(doc_pad, me // RING * WINDOW, 2 * WINDOW)
    doc_rows = doc_rows.reshape(8, T).astype(F32)
    ext = lax.dynamic_slice_in_dim(doc_pad, me * T + WINDOW - 3, T + 3)
    doc = ext[3:]
    docc = jnp.stack(
        [doc, doc == ext[2], doc == doc[T - 1]]
        + [doc == ext[3 - k : 3 - k + T] for k in range(1, 4)]
        + [doc, doc]
    ).astype(F32)
    shared = (
        conv_input, tail, gate_input, mix_grad, conv_weight, step_raw, step_bias[None],
        rate_log[None], docc, input_coeff, output_coeff,
    )
    act_t, g_t, loc, thr = phase_a(*shared)
    states = chain(loc.reshape(NH, 64, 128), thr).reshape(NH * 64, 128)
    outs = attn_core(kv, qd, halo, doc_rows)
    own = [ring_shift(outs[k], k) for k in range(RING)]
    back = [group_shift(outs[4 + k], k, -1) for k in range(RING)]
    dconv, dgate, spill, last, red, gstep, scal, coef = phase_b(
        *shared, act_t, g_t, states, skip_gain
    )
    dw, sc, gin, gout, fix = sums(red, scal, coef, spill, last)
    dconv = lax.dynamic_update_slice(dconv, fix.astype(BF16), (T - 8, 0))
    gq, gk, gv = attn_final(own, back)
    return (
        gq, gk, gv, dconv, dgate, gstep, gin, gout, dw, sc[0, :NH], sc[1, :NH], sc[2, :NH]
    )


def solution(mesh):
    both = P("seq", "head")
    return jax.shard_map(
        local,
        mesh=mesh,
        in_specs=(
            both, both, both, both, P(), both, P(None, "head"), both, P("head"), P("head"),
            P("head"), P("seq", None), P("seq", None), both, both,
        ),
        out_specs=(
            both, both, both, both, both, both, P("seq", None), P("seq", None),
            P(None, "head"), P("head"), P("head"), P("head"),
        ),
        check_vma=False,
    )
```

```python
import jax
import jax.numpy as jnp
from jax import lax
from jax.experimental import pallas as pl
from jax.experimental.pallas import tpu as pltpu
from jax.sharding import PartitionSpec as P

HEAD_DIM = 224
WINDOW = 1024
SSM_HEADS = 112
STATE = 64
GROUPS = 2
T = 256
NH = 28
PAIRS = 14
NSEQ = 32
RING = 4
NEG = -1e30
F32 = jnp.float32
BF16 = jnp.bfloat16
MESH = pl.DeviceIdType.MESH
VM = pltpu.VMEM
SCALE = HEAD_DIM ** (-0.5)
HI = lax.Precision.HIGHEST


def dot(a, b, ca, cb, precision=None):
    return lax.dot_general(
        a, b, (((ca,), (cb,)), ((), ())), preferred_element_type=F32, precision=precision
    )


def sigmoid(v):
    return 1.0 / (1.0 + jnp.exp(-v))


def col_of(row, rows):
    return jnp.transpose(jnp.broadcast_to(row, (rows, row.shape[1])))


def attn_kernel(*refs):
    kv, qd, halo, doc_ref, own, back, akv, aqd, dka, dva, doq = refs
    x = lax.rem(lax.axis_index("seq"), RING)
    for k in range(RING):
        c = lax.rem(x - k + RING, RING)
        akv[RING + c] = kv[k][...]
        akv[c] = halo[k][...]
        aqd[c] = qd[k][...]
    dka[...] = jnp.zeros_like(dka)
    dva[...] = jnp.zeros_like(dva)
    row_i = lax.broadcasted_iota(jnp.int32, (T, T), 0)
    col_j = lax.broadcasted_iota(jnp.int32, (T, T), 1)

    def chunk(c, carry):
        qt = aqd[c, 0]
        gt = aqd[c, 1]
        q = jnp.transpose(qt.astype(F32)).astype(BF16)
        g = jnp.transpose(gt.astype(F32)).astype(BF16)
        dq_col = col_of(doc_ref[pl.ds(RING + c, 1), :], 128)
        dq_col = jnp.concatenate([dq_col, dq_col], axis=1)
        scores, masks = [], []
        row_max = None
        for b in range(RING + 1):
            s = dot(q, akv[c + b, 0], 1, 0) * SCALE
            ok = dq_col == doc_ref[pl.ds(c + b, 1), :]
            if b == 0:
                ok = ok & (col_j > row_i)
            if b == RING:
                ok = ok & (col_j <= row_i)
            s = jnp.where(ok, s, NEG)
            scores.append(s)
            masks.append(ok)
            m = jnp.max(s, axis=1, keepdims=True)
            row_max = m if row_max is None else jnp.maximum(row_max, m)
        row_sum = None
        for b in range(RING + 1):
            e = jnp.where(masks[b], jnp.exp(scores[b] - row_max), 0.0)
            scores[b] = e
            r = jnp.sum(e, axis=1, keepdims=True)
            row_sum = r if row_sum is None else row_sum + r
        inv = 1.0 / jnp.maximum(row_sum, 1.0)
        dprobs = []
        delta = None
        for b in range(RING + 1):
            p = scores[b] * inv
            scores[b] = p
            half = p.astype(BF16)
            dp = dot(g, akv[c + b, 1], 1, 0)
            dprobs.append(dp)
            r = jnp.sum(half.astype(F32) * dp, axis=1, keepdims=True)
            delta = r if delta is None else delta + r
            dva[c + b] = dva[c + b] + dot(gt, half, 1, 0)
        dqt = None
        for b in range(RING + 1):
            ds = (scores[b] * (dprobs[b] - delta)).astype(BF16)
            r = dot(akv[c + b, 0], ds, 1, 1)
            dqt = r if dqt is None else dqt + r
            dka[c + b] = dka[c + b] + dot(qt, ds, 1, 0)
        doq[c] = dqt
        return carry

    lax.fori_loop(0, RING, chunk, 0)
    for k in range(RING):
        c = lax.rem(x + k, RING)
        own[k, 0] = (doq[c] * SCALE).astype(BF16)
        own[k, 1] = (dka[RING + c] * SCALE).astype(BF16)
        own[k, 2] = dva[RING + c].astype(BF16)
        back[k, 0] = (dka[c] * SCALE).astype(BF16)
        back[k, 1] = dva[c].astype(BF16)


def attn_core(kv, qd, halo, doc_rows):
    return pl.pallas_call(
        attn_kernel,
        out_shape=[
            jax.ShapeDtypeStruct((RING, 3, HEAD_DIM, T), BF16),
            jax.ShapeDtypeStruct((RING, 2, HEAD_DIM, T), BF16),
        ],
        scratch_shapes=[
            VM((2 * RING, 2, HEAD_DIM, T), BF16),
            VM((RING, 2, HEAD_DIM, T), BF16),
            VM((2 * RING, HEAD_DIM, T), F32),
            VM((2 * RING, HEAD_DIM, T), F32),
            VM((RING, HEAD_DIM, T), F32),
        ],
        name="attn_core",
        cost_estimate=pl.CostEstimate(
            flops=3000000000, bytes_accessed=8000000, transcendentals=1400000
        ),
    )(kv, qd, halo, doc_rows)


def mixer_setup(raw_ref, bias_ref, rate_ref, docc_ref, rows, tri, scr, mk):
    scr[...] = jnp.zeros_like(scr)
    step = jnp.log(1.0 + jnp.exp(raw_ref[...] + bias_ref[...]))
    scr[:, 0:NH] = step
    rows[0] = jnp.transpose(scr[...])[0:32]
    scr[:, 0:NH] = -step * jnp.exp(rate_ref[...])
    ld = jnp.transpose(scr[...])[0:32]
    rows[1] = ld
    i = lax.broadcasted_iota(jnp.int32, (T, T), 0)
    j = lax.broadcasted_iota(jnp.int32, (T, T), 1)
    tri[...] = jnp.where(i <= j, 1.0, 0.0)
    cum = dot(ld, tri[...], 1, 0, HI)
    rows[2] = cum
    rows[3] = jnp.where(docc_ref[1:2, :] > 0.0, jnp.exp(cum), 0.0)
    rows[4] = jnp.where(
        docc_ref[2:3, :] > 0.0, jnp.exp(jnp.minimum(cum[:, T - 1 : T] - cum, 0.0)), 0.0
    )
    for k in range(3):
        mk[k] = col_of(docc_ref[3 + k : 4 + k, :], 128)


def pair_rows(rows, which, pair):
    a = rows[which, pl.ds(2 * pair, 1), :]
    b = rows[which, pl.ds(2 * pair + 1, 1), :]
    return jnp.concatenate(
        [jnp.broadcast_to(a, (64, T)), jnp.broadcast_to(b, (64, T))], axis=0
    )


def group_cols(ref, group):
    v = ref[...].astype(F32)
    return jnp.where(group == 0, v[:, 0:STATE], v[:, STATE:])


def conv_forward(x, tail, w_ref, mk, xs):
    xs[0:8, :] = tail
    xs[8 : 8 + T, :] = x
    pre = w_ref[0:1, :] * x
    for k in range(1, 4):
        pre = pre + w_ref[k : k + 1, :] * (mk[k - 1] * xs[8 - k : 8 - k + T, :])
    return pre


def seq_copy(src, dst, send, recv, peer):
    return pltpu.make_async_remote_copy(
        src_ref=src,
        dst_ref=dst,
        send_sem=send,
        recv_sem=recv,
        device_id={"seq": peer},
        device_id_type=MESH,
    )


def greet_seq(barrier, me):
    def greet(k, carry):
        peer = lax.rem(me + k, NSEQ)
        pl.semaphore_signal(barrier, inc=1, device_id={"seq": peer}, device_id_type=MESH)
        return carry

    lax.fori_loop(1, NSEQ, greet, 0)


def tail_rows(ref, pair):
    lanes = pl.ds(pl.multiple_of(pair * 128, 128), 128)
    return ref[:, lanes].astype(F32)[8:16]


def front_kernel(
    conv_ref, gate_ref, mix_ref, w_ref, raw_ref, bias_ref, rate_ref, docc_ref, bin_ref, cout_ref,
    q_ref, k_ref, v_ref, do_ref, edge_ref,
    act_out, g_out, st_out, tail_out, kv_out, qd_out, halo_out,
    rows, tri, scr, mk, xs, bg, cg, kvp, qdp, tscr, tail_in, pay, inbox, outb, landed,
    hs, hr, ks, kr, qs, qr, ts, tr, ls, s1, r1, s2, r2,
):
    pair = pl.program_id(0)
    me = lax.axis_index("seq")
    x_me = lax.rem(me, RING)
    base = me - x_me
    fwd = lax.rem(base + RING, NSEQ)

    def halo_copy(k):
        return seq_copy(
            kvp.at[k], halo_out.at[k], hs.at[k], hr.at[k], fwd + lax.rem(x_me + k, RING)
        )

    def own_copy(k, src, dst, send, recv):
        return seq_copy(
            src.at[k], dst.at[k], send.at[k], recv.at[k], base + lax.rem(x_me + k, RING)
        )

    def stay(src, dst, i):
        return pltpu.make_async_copy(src.at[0], dst.at[0], ls.at[i])

    tail_copy = seq_copy(edge_ref, tail_in, ts, tr, lax.rem(me + 1, NSEQ))

    @pl.when(pair == 0)
    def _():
        barrier = pltpu.get_barrier_semaphore()
        greet_seq(barrier, me)
        for slot, (src, dest) in enumerate(((k_ref, kvp), (v_ref, kvp), (q_ref, qdp), (do_ref, qdp))):
            tscr[...] = jnp.transpose(src[...].astype(F32)).astype(BF16)
            for k in range(RING):
                h = lax.rem(x_me + k, RING)
                dest[k, slot % 2] = tscr[pl.ds(pl.multiple_of(h * HEAD_DIM, 32), HEAD_DIM), :]
        pl.semaphore_wait(barrier, NSEQ - 1)
        tail_copy.start()
        for k in range(RING):
            halo_copy(k).start()
            if k:
                own_copy(k, kvp, kv_out, ks, kr).start()
        stay(kvp, kv_out, 0).start()
        stay(qdp, qd_out, 1).start()
        mixer_setup(raw_ref, bias_ref, rate_ref, docc_ref, rows, tri, scr, mk)
        group = lax.axis_index("head") // 2
        bg[...] = group_cols(bin_ref, group).astype(BF16)
        cg[...] = group_cols(cout_ref, group).astype(BF16)
        thr = rows[3][:, T - 1 : T]
        for e in range(NH):
            t = jnp.broadcast_to(thr[e : e + 1, :], (8, 128))
            hi = t.astype(BF16).astype(F32)
            pay[e, 64:80, :] = jnp.concatenate([hi, t - hi], axis=0).astype(BF16)
        tail_copy.wait_recv()
        tail_out[...] = tail_in[...]

    x = conv_ref[...].astype(F32)
    pre = conv_forward(x, tail_rows(tail_in, pair), w_ref, mk, xs)
    act = pre * sigmoid(pre)
    gate = gate_ref[...].astype(F32)
    g = mix_ref[...].astype(F32) * (gate * sigmoid(gate))
    act_t = jnp.transpose(act)
    g_t = jnp.transpose(g)
    act_out[...] = act_t
    g_out[...] = g_t
    st = act_t * (pair_rows(rows, 0, pair) * pair_rows(rows, 4, pair))
    ge = g_t * pair_rows(rows, 3, pair)
    both = jnp.concatenate(
        [dot(st.astype(BF16), bg[...], 1, 0), dot(ge.astype(BF16), cg[...], 1, 0)], axis=1
    ).astype(BF16)
    pay[2 * pair, 0:64, :] = both[0:64]
    pay[2 * pair + 1, 0:64, :] = both[64:128]

    def first(peer, frm):
        return seq_copy(pay.at[peer], inbox.at[frm], s1.at[peer], r1.at[frm], peer)

    def second(peer, frm):
        return seq_copy(outb.at[peer], landed.at[frm], s2.at[peer], r2.at[frm], peer)

    @pl.when(pair == PAIRS - 1)
    def _():
        def send_first(k, carry):
            peer = lax.rem(me + k, NSEQ)

            @pl.when(peer < NH)
            def _():
                first(peer, me).start()

            return carry

        lax.fori_loop(1, NSEQ, send_first, 0)
        for k in range(1, RING):
            own_copy(k, qdp, qd_out, qs, qr).start()

        @pl.when(me < NH)
        def _():
            inbox[me] = pay[me]

            def wait_first(k, carry):
                first(me, lax.rem(me + k, NSEQ)).wait_recv()
                return carry

            lax.fori_loop(1, NSEQ, wait_first, 0)
            lane = lax.broadcasted_iota(jnp.int32, (64, 128), 1)

            def gain(s):
                tail = inbox[s, 64:80, :].astype(F32)
                return tail[0:1] + tail[8:9]

            def down(s, run):
                outb[s] = run.astype(BF16)
                return gain(s) * run + inbox[s, 0:64, :].astype(F32)

            lax.fori_loop(0, NSEQ, down, jnp.zeros((64, 128), F32))

            def up(k, run):
                s = NSEQ - 1 - k
                outb[s] = jnp.where(lane < STATE, outb[s].astype(F32), run).astype(BF16)
                return gain(s) * run + inbox[s, 0:64, :].astype(F32)

            lax.fori_loop(0, NSEQ, up, jnp.zeros((64, 128), F32))

            def send_second(k, carry):
                second(lax.rem(me + k, NSEQ), me).start()
                return carry

            lax.fori_loop(1, NSEQ, send_second, 0)
            landed[me] = outb[me]

        def finish(k, carry):
            peer = lax.rem(me + k, NSEQ)

            @pl.when(peer < NH)
            def _():
                first(peer, me).wait_send()
                second(me, peer).wait_recv()

            return carry

        lax.fori_loop(1, NSEQ, finish, 0)

        @pl.when(me < NH)
        def _():
            def drain(k, carry):
                second(lax.rem(me + k, NSEQ), me).wait_send()
                return carry

            lax.fori_loop(1, NSEQ, drain, 0)

        for e in range(NH):
            st_out[64 * e : 64 * e + 64, :] = landed[e]
        tail_copy.wait_send()
        stay(kvp, kv_out, 0).wait()
        stay(qdp, qd_out, 1).wait()
        for k in range(RING):
            halo_copy(k).wait()
            if k:
                own_copy(k, kvp, kv_out, ks, kr).wait()
                own_copy(k, qdp, qd_out, qs, qr).wait()


def whole_spec(shape):
    return pl.BlockSpec(shape, lambda i: (0,) * len(shape))


def mixer_specs():
    tok = pl.BlockSpec((T, 128), lambda i: (0, i))
    return [
        tok,
        tok,
        tok,
        pl.BlockSpec((4, 128), lambda i: (0, i)),
        whole_spec((T, NH)),
        whole_spec((1, NH)),
        whole_spec((1, NH)),
        whole_spec((8, T)),
        whole_spec((T, 128)),
        whole_spec((T, 128)),
    ]


DMA = pltpu.SemaphoreType.DMA
WIDTH = NH * 64
ANY = pl.BlockSpec(memory_space=pl.ANY)


def front(shared, queries, keys, values, attn_grad):
    chan = pl.BlockSpec((128, T), lambda i: (i, 0))
    piece = jax.ShapeDtypeStruct((RING, 2, HEAD_DIM, T), BF16)
    return pl.pallas_call(
        front_kernel,
        grid=(PAIRS,),
        in_specs=mixer_specs()
        + [whole_spec((T, 4 * HEAD_DIM))] * 4
        + [pl.BlockSpec((16, WIDTH), lambda i: (T // 16 - 1, 0))],
        out_specs=[chan, chan, whole_spec((WIDTH, 128)), whole_spec((16, WIDTH)), ANY, ANY, ANY],
        out_shape=[
            jax.ShapeDtypeStruct((WIDTH, T), F32),
            jax.ShapeDtypeStruct((WIDTH, T), F32),
            jax.ShapeDtypeStruct((WIDTH, 128), BF16),
            jax.ShapeDtypeStruct((16, WIDTH), BF16),
            piece,
            piece,
            piece,
        ],
        scratch_shapes=[
            VM((5, 32, T), F32),
            VM((T, T), F32),
            VM((T, 128), F32),
            VM((3, T, 128), F32),
            VM((8 + T, 128), F32),
            VM((T, STATE), BF16),
            VM((T, STATE), BF16),
            VM((RING, 2, HEAD_DIM, T), BF16),
            VM((RING, 2, HEAD_DIM, T), BF16),
            VM((4 * HEAD_DIM, T), BF16),
            VM((16, WIDTH), BF16),
            VM((NH, 80, 128), BF16),
            VM((NSEQ, 80, 128), BF16),
            VM((NSEQ, 64, 128), BF16),
            VM((NH, 64, 128), BF16),
            DMA((RING,)), DMA((RING,)), DMA((RING,)), DMA((RING,)), DMA((RING,)), DMA((RING,)),
            DMA, DMA, DMA((2,)), DMA((NSEQ,)), DMA((NSEQ,)), DMA((NSEQ,)), DMA((NSEQ,)),
        ],
        compiler_params=pltpu.CompilerParams(collective_id=1, has_side_effects=True),
        name="front",
        cost_estimate=pl.CostEstimate(
            flops=600000000, bytes_accessed=12000000, transcendentals=1000000
        ),
    )(*shared, queries, keys, values, attn_grad, shared[0])


def rear_kernel(
    conv_ref, gate_ref, mix_ref, w_ref, raw_ref, bias_ref, rate_ref, docc_ref, bin_ref, cout_ref,
    act_ref, g_ref, st_ref, skip_ref, tail_ref, own_ref, back_ref,
    dconv_out, dgate_out, step_out, dw_out, sc_out, gin_out, gout_out, gq_out, gk_out, gv_out,
    rows, tri, scr, mk, xs, bg, cg, bias_m, pair_t, dpair, dcum, ddir, dskp, dbt, dct, qs,
    last, spill, spin, red, inbox, tot, coef_ref, cin, own_in, back_in, fscr,
    bs, br, os, orr, s1, r1, s2, r2, s3, r3, s4, r4,
):
    pair = pl.program_id(0)
    me = lax.axis_index("seq")
    hd = lax.axis_index("head")
    x_me = lax.rem(me, RING)
    base = me - x_me
    bwd = lax.rem(base + NSEQ - RING, NSEQ)

    def back_copy(k):
        return seq_copy(
            back_ref.at[k], back_in.at[k], bs.at[k], br.at[k], bwd + lax.rem(x_me + k, RING)
        )

    def own_copy(k):
        return seq_copy(
            own_ref.at[k], own_in.at[k], os.at[k], orr.at[k], base + lax.rem(x_me + k, RING)
        )

    @pl.when(pair == 0)
    def _():
        barrier = pltpu.get_barrier_semaphore()
        greet_seq(barrier, me)
        for k in range(1, 4):
            pl.semaphore_signal(
                barrier, inc=1, device_id={"head": lax.rem(hd + k, 4)}, device_id_type=MESH
            )
        pl.semaphore_wait(barrier, NSEQ + 2)
        for k in range(RING):
            back_copy(k).start()
            if k:
                own_copy(k).start()
        pltpu.make_async_copy(own_ref.at[0], own_in.at[0], os.at[0]).start()
        red[...] = jnp.zeros_like(red)
        mixer_setup(raw_ref, bias_ref, rate_ref, docc_ref, rows, tri, scr, mk)
        group = lax.axis_index("head") // 2
        bf = group_cols(bin_ref, group)
        cf = group_cols(cout_ref, group)
        bg[...] = bf.astype(BF16)
        cg[...] = cf.astype(BF16)
        pair_t[...] = dot(bf, cf, 1, 1, HI)
        doc = docc_ref[0:1, :]
        dcol = col_of(doc, 128)
        dcol = jnp.concatenate([dcol, dcol], axis=1)
        ok = (tri[...] > 0.5) & (dcol == doc)
        bias_m[...] = jnp.where(ok, 0.0, NEG)
        dpair[...] = jnp.zeros_like(dpair)
        dbt[...] = jnp.zeros_like(dbt)
        dct[...] = jnp.zeros_like(dct)
        dcum[...] = jnp.zeros_like(dcum)
        ddir[...] = jnp.zeros_like(ddir)
        dskp[...] = jnp.zeros_like(dskp)
        qs[...] = jnp.zeros_like(qs)

    act_t = act_ref[...]
    g_t = g_ref[...]
    step_p = pair_rows(rows, 0, pair)
    eg_p = pair_rows(rows, 3, pair)
    te_p = pair_rows(rows, 4, pair)
    s_t = act_t * step_p
    s_b = s_t.astype(BF16)
    g_b = g_t.astype(BF16)
    state = st_ref[...]
    start = state[:, 0:STATE]
    end = state[:, STATE:]
    car = dot(start, cg[...], 1, 1) * eg_p
    dste = dot(end, bg[...], 1, 1) * te_p
    dct[...] += dot(start, (g_t * eg_p).astype(BF16), 0, 0)
    dbt[...] += dot(end, (s_t * te_p).astype(BF16), 0, 0)
    se = start.astype(F32) * end.astype(F32)
    lane = lax.broadcasted_iota(jnp.int32, (1, T), 1)
    ys, dss = [], []
    for a in range(2):
        lo = 64 * a
        h = 2 * pair + a
        cum = rows[2, pl.ds(h, 1), :]
        cc = col_of(cum, 128)
        cc = jnp.concatenate([cc, cc], axis=1)
        w = jnp.exp(jnp.minimum(cum - cc, 0.0) + bias_m[...])
        m = pair_t[...] * w
        mb = m.astype(BF16)
        sh = s_b[lo : lo + 64]
        gh = g_b[lo : lo + 64]
        y = dot(sh, mb, 1, 0)
        dsi = dot(gh, mb, 1, 1)
        dm = dot(sh, gh, 0, 0)
        dpair[...] += dm * w
        z = dm * m
        zr = jnp.sum(jnp.transpose(z[:, 0:128] + z[:, 128:]), axis=0, keepdims=True)
        carh = car[lo : lo + 64]
        dsth = dste[lo : lo + 64]
        gt = g_t[lo : lo + 64]
        st = s_t[lo : lo + 64]
        at = act_t[lo : lo + 64]
        v = jnp.sum(st * dsth, axis=0, keepdims=True)
        d = jnp.sum(z, axis=0, keepdims=True) - zr + jnp.sum(gt * carh, axis=0, keepdims=True) - v
        thr = rows[3, pl.ds(h, 1), :][:, T - 1 : T]
        extra = jnp.sum(v, axis=1, keepdims=True) + thr * jnp.sum(
            jnp.sum(se[lo : lo + 64], axis=0, keepdims=True), axis=1, keepdims=True
        )
        dcum[pl.ds(h, 1), :] = d + jnp.where(lane == T - 1, extra, 0.0)
        ds = dsi + dsth
        ddir[pl.ds(h, 1), :] = jnp.sum(ds * at, axis=0, keepdims=True)
        dskp[pl.ds(h, 1), :] = jnp.sum(gt * at, axis=0, keepdims=True)
        skip = skip_ref[h]
        ys.append(y + carh + skip * at)
        dss.append(ds * step_p[lo : lo + 64] + skip * gt)
    y = jnp.transpose(jnp.concatenate(ys, axis=0))
    dact = jnp.transpose(jnp.concatenate(dss, axis=0))
    gate = gate_ref[...].astype(F32)
    sg = sigmoid(gate)
    dgate_out[...] = (
        mix_ref[...].astype(F32) * y * (sg * (1.0 + gate * (1.0 - sg)))
    ).astype(BF16)
    x = conv_ref[...].astype(F32)
    pre = conv_forward(x, tail_rows(tail_ref, pair), w_ref, mk, xs)
    sp = sigmoid(pre)
    dpre = dact * (sp * (1.0 + pre * (1.0 - sp)))
    dx = None
    for k in range(4):
        q = dpre if k == 0 else dpre * mk[k - 1]
        red[pair, k : k + 1, :] = jnp.sum(q * xs[8 - k : 8 - k + T, :], axis=0, keepdims=True)
        qs[8 : 8 + T, :] = q
        term = w_ref[k : k + 1, :] * qs[k : k + 8 + T, :]
        dx = term if dx is None else dx + term
    lanes = pl.ds(pl.multiple_of(pair * 128, 128), 128)
    spill[:, lanes] = dx[0:8]
    dconv_out[:, lanes] = dx[8:].astype(BF16)
    last[:, lanes] = dx[T - 8 :]

    @pl.when(pair == PAIRS - 1)
    def _():
        dld = dot(dcum[...], tri[...], 1, 1, HI)
        zero = jnp.zeros((96, T), F32)
        to_tok = lambda v: jnp.transpose(jnp.concatenate([v, zero], axis=0))[:, 0:NH]
        dld_t = to_tok(dld)
        dir_t = to_tok(ddir[...])
        rate = jnp.exp(rate_ref[...])
        v = raw_ref[...] + bias_ref[...]
        step = jnp.log(1.0 + jnp.exp(v))
        gs = (dir_t - dld_t * rate) * sigmoid(v)
        step_out[...] = gs
        red[PAIRS, 0:1, 0:NH] = jnp.sum(gs, axis=0, keepdims=True)
        red[PAIRS, 1:2, 0:NH] = -rate * jnp.sum(dld_t * step, axis=0, keepdims=True)
        red[PAIRS, 2:3, 0:NH] = jnp.sum(to_tok(dskp[...]), axis=0, keepdims=True)
        dp = dpair[...].astype(BF16)
        coef_ref[0:STATE] = (dbt[...] + dot(jnp.transpose(cg[...].astype(F32)).astype(BF16), dp, 1, 1)).astype(BF16)
        coef_ref[STATE:] = (dct[...] + dot(jnp.transpose(bg[...].astype(F32)).astype(BF16), dp, 1, 0)).astype(BF16)

        def coef(k, frm):
            return pltpu.make_async_remote_copy(
                src_ref=coef_ref,
                dst_ref=cin.at[frm],
                send_sem=s3.at[k],
                recv_sem=r3.at[frm],
                device_id={"head": lax.rem(hd + k, 4)},
                device_id_type=MESH,
            )

        spill_copy = seq_copy(spill, spin, s4, r4, lax.rem(me + NSEQ - 1, NSEQ))

        def first(block, frm):
            return seq_copy(red.at[block], inbox.at[frm], s1.at[block], r1.at[frm], 2 * block)

        def second(peer, block):
            return seq_copy(tot.at[block], tot.at[block], s2.at[peer], r2.at[block], peer)

        def send_first(b, carry):
            @pl.when(2 * b != me)
            def _():
                first(b, me).start()

            return carry

        lax.fori_loop(0, BLOCKS, send_first, 0)
        for k in range(1, 4):
            coef(k, hd).start()
        spill_copy.start()
        mine = me // 2
        owner = (me == 2 * mine) & (mine < BLOCKS)

        @pl.when(owner)
        def _():
            inbox[me] = red[mine]

            def wait_first(k, carry):
                first(mine, lax.rem(me + k, NSEQ)).wait_recv()
                return carry

            lax.fori_loop(1, NSEQ, wait_first, 0)
            tot[mine] = jnp.sum(inbox[...], axis=0)

            def send_second(k, carry):
                second(lax.rem(me + k, NSEQ), mine).start()
                return carry

            lax.fori_loop(1, NSEQ, send_second, 0)

        for k in range(1, 4):
            coef(k, lax.rem(hd + k, 4)).wait_recv()
        cin[hd] = coef_ref[...]
        g0 = jnp.transpose(cin[0].astype(F32) + cin[1].astype(F32))
        g1 = jnp.transpose(cin[2].astype(F32) + cin[3].astype(F32))
        gin_out[...] = jnp.concatenate([g0[:, 0:STATE], g1[:, 0:STATE]], axis=1)
        gout_out[...] = jnp.concatenate([g0[:, STATE:], g1[:, STATE:]], axis=1)
        spill_copy.wait_recv()
        fixed = jnp.concatenate([last[0:8, :], last[8:16, :] + spin[...]], axis=0)
        dconv_out[T - 16 :, :] = fixed.astype(BF16)
        pltpu.make_async_copy(own_ref.at[0], own_in.at[0], os.at[0]).wait()
        for k in range(RING):
            if k:
                own_copy(k).wait()
            back_copy(k).wait()
        for slot, dest in enumerate((gq_out, gk_out, gv_out)):
            for k in range(RING):
                h = lax.rem(x_me - k + RING, RING)
                part = own_in[k, slot].astype(F32)
                if slot:
                    part = part + back_in[k, slot - 1].astype(F32)
                fscr[pl.ds(pl.multiple_of(h * HEAD_DIM, 32), HEAD_DIM), :] = part
            dest[...] = jnp.transpose(fscr[...]).astype(BF16)

        def wait_second(b, carry):
            @pl.when(2 * b != me)
            def _():
                second(me, b).wait_recv()
                first(b, me).wait_send()

            return carry

        lax.fori_loop(0, BLOCKS, wait_second, 0)
        for p in range(PAIRS):
            dw_out[:, 128 * p : 128 * p + 128] = tot[p, 0:4, :]
        sc_out[...] = tot[PAIRS]

        @pl.when(owner)
        def _():
            def drain(k, carry):
                second(lax.rem(me + k, NSEQ), mine).wait_send()
                return carry

            lax.fori_loop(1, NSEQ, drain, 0)

        for k in range(1, 4):
            coef(k, hd).wait_send()
        spill_copy.wait_send()


BLOCKS = PAIRS + 1


def rear(shared, act_t, g_t, states, skip, tail, own, back):
    tok = pl.BlockSpec((T, 128), lambda i: (0, i))
    chan = pl.BlockSpec((128, T), lambda i: (i, 0))
    piece = jax.ShapeDtypeStruct((T, 4 * HEAD_DIM), BF16)
    outs = [
        jax.ShapeDtypeStruct((T, WIDTH), BF16),
        jax.ShapeDtypeStruct((T, WIDTH), BF16),
        jax.ShapeDtypeStruct((T, NH), F32),
        jax.ShapeDtypeStruct((4, WIDTH), F32),
        jax.ShapeDtypeStruct((8, 128), F32),
        jax.ShapeDtypeStruct((T, 128), F32),
        jax.ShapeDtypeStruct((T, 128), F32),
        piece,
        piece,
        piece,
    ]
    specs = [whole_spec(o.shape) for o in outs]
    specs[1] = tok
    return pl.pallas_call(
        rear_kernel,
        grid=(PAIRS,),
        in_specs=mixer_specs()
        + [
            chan,
            chan,
            pl.BlockSpec((128, 128), lambda i: (i, 0)),
            pl.BlockSpec(memory_space=pltpu.SMEM),
            whole_spec((16, WIDTH)),
            ANY,
            ANY,
        ],
        out_specs=specs,
        out_shape=outs,
        scratch_shapes=[
            VM((5, 32, T), F32),
            VM((T, T), F32),
            VM((T, 128), F32),
            VM((3, T, 128), F32),
            VM((8 + T, 128), F32),
            VM((T, STATE), BF16),
            VM((T, STATE), BF16),
            VM((T, T), F32),
            VM((T, T), F32),
            VM((T, T), F32),
            VM((32, T), F32),
            VM((32, T), F32),
            VM((32, T), F32),
            VM((STATE, T), F32),
            VM((STATE, T), F32),
            VM((16 + T, 128), F32),
            VM((16, WIDTH), F32),
            VM((8, WIDTH), F32),
            VM((8, WIDTH), F32),
            VM((BLOCKS, 8, 128), F32),
            VM((NSEQ, 8, 128), F32),
            VM((BLOCKS, 8, 128), F32),
            VM((128, T), BF16),
            VM((4, 128, T), BF16),
            VM((RING, 3, HEAD_DIM, T), BF16),
            VM((RING, 2, HEAD_DIM, T), BF16),
            VM((4 * HEAD_DIM, T), F32),
            DMA((RING,)), DMA((RING,)), DMA((RING,)), DMA((RING,)),
            DMA((BLOCKS,)), DMA((NSEQ,)), DMA((NSEQ,)), DMA((BLOCKS,)),
            DMA((4,)), DMA((4,)), DMA, DMA,
        ],
        compiler_params=pltpu.CompilerParams(collective_id=2, has_side_effects=True),
        name="rear",
        cost_estimate=pl.CostEstimate(
            flops=3000000000, bytes_accessed=10000000, transcendentals=3000000
        ),
    )(*shared, act_t, g_t, states, skip, tail, own, back)


def local(
    queries, keys, values, attn_grad, doc_ids, conv_input, conv_weight, step_raw, step_bias,
    rate_log, skip_gain, input_coeff, output_coeff, gate_input, mix_grad,
):
    me = lax.axis_index("seq")
    doc_pad = jnp.concatenate([jnp.full((WINDOW,), -1, jnp.int32), doc_ids])
    doc_rows = lax.dynamic_slice_in_dim(doc_pad, me // RING * WINDOW, 2 * WINDOW)
    doc_rows = doc_rows.reshape(8, T).astype(F32)
    ext = lax.dynamic_slice_in_dim(doc_pad, me * T + WINDOW - 3, T + 3)
    doc = ext[3:]
    docc = jnp.stack(
        [doc, doc == ext[2], doc == doc[T - 1]]
        + [doc == ext[3 - k : 3 - k + T] for k in range(1, 4)]
        + [doc, doc]
    ).astype(F32)
    shared = (
        conv_input, gate_input, mix_grad, conv_weight, step_raw, step_bias[None], rate_log[None],
        docc, input_coeff, output_coeff,
    )
    act_t, g_t, states, tail, kv, qd, halo = front(shared, queries, keys, values, attn_grad)
    own, back = attn_core(kv, qd, halo, doc_rows)
    dconv, dgate, gstep, dw, sc, gin, gout, gq, gk, gv = rear(
        shared, act_t, g_t, states, skip_gain, tail, own, back
    )
    return (
        gq, gk, gv, dconv, dgate, gstep, gin, gout, dw, sc[0, :NH], sc[1, :NH], sc[2, :NH]
    )


def solution(mesh):
    both = P("seq", "head")
    return jax.shard_map(
        local,
        mesh=mesh,
        in_specs=(
            both, both, both, both, P(), both, P(None, "head"), both, P("head"), P("head"),
            P("head"), P("seq", None), P("seq", None), both, both,
        ),
        out_specs=(
            both, both, both, both, both, both, P("seq", None), P("seq", None),
            P(None, "head"), P("head"), P("head"), P("head"),
        ),
        check_vma=False,
    )
```

```python
import jax
import jax.numpy as jnp
from jax import lax
from jax.experimental import pallas as pl
from jax.experimental.pallas import tpu as pltpu
from jax.sharding import PartitionSpec as P

HEAD_DIM = 224
WINDOW = 1024
SSM_HEADS = 112
STATE = 64
GROUPS = 2
T = 256
NH = 28
PAIRS = 14
NSEQ = 32
RING = 4
NEG = -1e30
F32 = jnp.float32
BF16 = jnp.bfloat16
MESH = pl.DeviceIdType.MESH
VM = pltpu.VMEM
SCALE = HEAD_DIM ** (-0.5)
HI = lax.Precision.HIGHEST


def dot(a, b, ca, cb, precision=None):
    return lax.dot_general(
        a, b, (((ca,), (cb,)), ((), ())), preferred_element_type=F32, precision=precision
    )


def sigmoid(v):
    return 1.0 / (1.0 + jnp.exp(-v))


def col_of(row, rows):
    return jnp.transpose(jnp.broadcast_to(row, (rows, row.shape[1])))


DMA = pltpu.SemaphoreType.DMA
WIDTH = NH * 64
BLOCKS = PAIRS + 1
ANY = pl.BlockSpec(memory_space=pl.ANY)


def doc_row(ref, shard):
    safe = jnp.maximum(shard, 0) * 2
    row = jnp.concatenate([ref[pl.ds(safe, 1), :], ref[pl.ds(safe + 1, 1), :]], axis=1)
    return jnp.where(shard < 0, -1.0, row.astype(F32))


def mixer_setup(me, raw_ref, bias_ref, rate_ref, doc_ref, drows, rows, tri, mk, vcol, small):
    base = me - lax.rem(me, RING)
    for c in range(2 * RING):
        drows[c : c + 1, :] = doc_row(doc_ref, base - RING + c)
    doc = doc_row(doc_ref, me)
    prev = doc_row(doc_ref, me - 1)
    small[...] = jnp.zeros_like(small)
    small[0:1, 0:NH] = bias_ref[...]
    small[1:2, 0:NH] = jnp.exp(rate_ref[...])
    bias = col_of(small[0:1, :], 128)[0:NH]
    rate = col_of(small[1:2, :], 128)[0:NH]
    vcol[...] = jnp.concatenate([rate, rate], axis=1)
    rows[...] = jnp.zeros_like(rows)
    step = jnp.log(1.0 + jnp.exp(raw_ref[...] + jnp.concatenate([bias, bias], axis=1)))
    rows[0, 0:NH, :] = step
    rows[1, 0:NH, :] = -step * vcol[...]
    i = lax.broadcasted_iota(jnp.int32, (T, T), 0)
    j = lax.broadcasted_iota(jnp.int32, (T, T), 1)
    tri[...] = jnp.where(i <= j, 1.0, 0.0)
    cum = dot(rows[1], tri[...], 1, 0, HI)
    rows[2] = cum
    rows[3] = jnp.where(doc == prev[:, T - 1 : T], jnp.exp(cum), 0.0)
    rows[4] = jnp.where(
        doc == doc[:, T - 1 : T], jnp.exp(jnp.minimum(cum[:, T - 1 : T] - cum, 0.0)), 0.0
    )
    lane = lax.broadcasted_iota(jnp.int32, (8, T), 1)
    doc8 = jnp.broadcast_to(doc, (8, T))
    prev8 = jnp.broadcast_to(prev, (8, T))
    for k in range(1, 4):
        lag = jnp.where(lane < k, pltpu.roll(prev8, k, 1), pltpu.roll(doc8, k, 1))
        mk[k - 1] = col_of(jnp.where(lag == doc8, 1.0, 0.0)[0:1, :], 128)


def pair_rows(rows, which, pair):
    a = rows[which, pl.ds(2 * pair, 1), :]
    b = rows[which, pl.ds(2 * pair + 1, 1), :]
    return jnp.concatenate(
        [jnp.broadcast_to(a, (64, T)), jnp.broadcast_to(b, (64, T))], axis=0
    )


def group_cols(ref, group):
    v = ref[...].astype(F32)
    return jnp.where(group == 0, v[:, 0:STATE], v[:, STATE:])


def conv_forward(x, tail, w_ref, mk, xs):
    xs[0:8, :] = tail
    xs[8 : 8 + T, :] = x
    pre = w_ref[0:1, :] * x
    for k in range(1, 4):
        pre = pre + w_ref[k : k + 1, :] * (mk[k - 1] * xs[8 - k : 8 - k + T, :])
    return pre


def tail_rows(ref, pair):
    lanes = pl.ds(pl.multiple_of(pair * 128, 128), 128)
    return ref[:, lanes].astype(F32)[8:16]


def seq_copy(src, dst, send, recv, peer):
    return pltpu.make_async_remote_copy(
        src_ref=src,
        dst_ref=dst,
        send_sem=send,
        recv_sem=recv,
        device_id={"seq": peer},
        device_id_type=MESH,
    )


def greet_seq(barrier, me):
    def greet(k, carry):
        peer = lax.rem(me + k, NSEQ)
        pl.semaphore_signal(barrier, inc=1, device_id={"seq": peer}, device_id_type=MESH)
        return carry

    lax.fori_loop(1, NSEQ, greet, 0)


def attention(x_me, kva, qda, drows, dka, dva, dq_out, send_dq):
    dka[...] = jnp.zeros_like(dka)
    dva[...] = jnp.zeros_like(dva)
    row_i = lax.broadcasted_iota(jnp.int32, (T, T), 0)
    col_j = lax.broadcasted_iota(jnp.int32, (T, T), 1)

    def chunk(c, carry):
        slot = lax.rem(x_me - c + RING, RING)
        qt = qda[slot, 0]
        gt = qda[slot, 1]
        q = jnp.transpose(qt.astype(F32)).astype(BF16)
        g = jnp.transpose(gt.astype(F32)).astype(BF16)
        dq_col = col_of(drows[pl.ds(RING + c, 1), :], 128)
        dq_col = jnp.concatenate([dq_col, dq_col], axis=1)
        scores, masks, slots = [], [], []
        row_max = None
        for b in range(RING + 1):
            kc = c + b
            slots.append(kc // RING * RING + lax.rem(x_me - kc + 2 * RING, RING))
            s = dot(q, kva[slots[b], 0], 1, 0) * SCALE
            ok = dq_col == drows[pl.ds(kc, 1), :]
            if b == 0:
                ok = ok & (col_j > row_i)
            if b == RING:
                ok = ok & (col_j <= row_i)
            s = jnp.where(ok, s, NEG)
            scores.append(s)
            masks.append(ok)
            m = jnp.max(s, axis=1, keepdims=True)
            row_max = m if row_max is None else jnp.maximum(row_max, m)
        row_sum = None
        for b in range(RING + 1):
            e = jnp.where(masks[b], jnp.exp(scores[b] - row_max), 0.0)
            scores[b] = e
            r = jnp.sum(e, axis=1, keepdims=True)
            row_sum = r if row_sum is None else row_sum + r
        inv = 1.0 / jnp.maximum(row_sum, 1.0)
        dprobs = []
        delta = None
        for b in range(RING + 1):
            p = scores[b] * inv
            scores[b] = p
            half = p.astype(BF16)
            dp = dot(g, kva[slots[b], 1], 1, 0)
            dprobs.append(dp)
            r = jnp.sum(half.astype(F32) * dp, axis=1, keepdims=True)
            delta = r if delta is None else delta + r
            dva[c + b] = dva[c + b] + dot(gt, half, 1, 0)
        dqt = None
        for b in range(RING + 1):
            ds = (scores[b] * (dprobs[b] - delta)).astype(BF16)
            r = dot(kva[slots[b], 0], ds, 1, 1)
            dqt = r if dqt is None else dqt + r
            dka[c + b] = dka[c + b] + dot(qt, ds, 1, 0)
        k = lax.rem(c - x_me + RING, RING)
        dq_out[k] = (dqt * SCALE).astype(BF16)
        send_dq(k)
        return carry

    lax.fori_loop(0, RING, chunk, 0)


def layer_kernel(
    conv_ref, gate_ref, mix_ref, w_ref, raw_ref, bias_ref, rate_ref, doc_ref, bin_ref, cout_ref,
    q_ref, k_ref, v_ref, do_ref, edge_ref, skip_ref,
    dconv_out, dgate_out, step_out, dw_out, sc_out, gin_out, gout_out, gq_out, gk_out, gv_out,
    drows, rows, tri, mk, vcol, small, xs, bg, cg, act_s, g_s,
    kvp, qdp, tscr, kva, qda, tail_in, pay, inbox, outb, landed,
    dka, dva, dq_out, own_out, back_out, dq_in, own_in, back_in, fscr,
    bias_m, pair_t, dpair, dcum, ddir, dskp, dbt, dct, qs,
    last, spill, spin, red, rinbox, tot, coef_ref, cin,
    hs, hr, ks, kr, qsm, qr, ts, tr, cs1, cr1, cs2, cr2,
    ds_, dr, osm, orr, bs, br, s1, r1, s2, r2, s3, r3, s4, r4,
):
    step_id = pl.program_id(0)
    pair = lax.rem(step_id, PAIRS)
    me = lax.axis_index("seq")
    hd = lax.axis_index("head")
    x_me = lax.rem(me, RING)
    base = me - x_me
    fwd = lax.rem(base + RING, NSEQ)
    bwd = lax.rem(base + NSEQ - RING, NSEQ)

    def near(k):
        return base + lax.rem(x_me + k, RING)

    def halo_copy(k):
        return seq_copy(kva.at[RING + k], kva.at[k], hs.at[k], hr.at[k], fwd + x_me)

    def kv_copy(k):
        return seq_copy(kvp.at[k], kva.at[RING + k], ks.at[k], kr.at[k], near(k))

    def qd_copy(k):
        return seq_copy(qdp.at[k], qda.at[k], qsm.at[k], qr.at[k], near(k))

    def dq_copy(k):
        return seq_copy(dq_out.at[k], dq_in.at[k], ds_.at[k], dr.at[k], near(k))

    def own_copy(k):
        return seq_copy(own_out.at[k], own_in.at[k], osm.at[k], orr.at[k], near(k))

    def back_copy(k):
        return seq_copy(
            back_out.at[k], back_in.at[k], bs.at[k], br.at[k], bwd + lax.rem(x_me + k, RING)
        )

    def first_copy(peer, frm):
        return seq_copy(pay.at[peer], inbox.at[frm], cs1.at[peer], cr1.at[frm], peer)

    def second_copy(peer, frm):
        return seq_copy(outb.at[peer], landed.at[frm], cs2.at[peer], cr2.at[frm], peer)

    tail_copy = seq_copy(edge_ref, tail_in, ts, tr, lax.rem(me + 1, NSEQ))

    @pl.when(step_id == 0)
    def _():
        barrier = pltpu.get_barrier_semaphore()
        greet_seq(barrier, me)
        for k in range(1, 4):
            pl.semaphore_signal(
                barrier, inc=1, device_id={"head": lax.rem(hd + k, 4)}, device_id_type=MESH
            )

        def prepare(src, dest, landing, slot):
            tscr[...] = jnp.transpose(src[...].astype(F32)).astype(BF16)
            for k in range(RING):
                h = lax.rem(x_me + k, RING)
                part = tscr[pl.ds(pl.multiple_of(h * HEAD_DIM, 32), HEAD_DIM), :]
                if k:
                    dest[k, slot] = part
                else:
                    landing[slot] = part

        prepare(k_ref, kvp, kva.at[RING], 0)
        prepare(v_ref, kvp, kva.at[RING], 1)
        pl.semaphore_wait(barrier, NSEQ + 2)
        tail_copy.start()
        halo_copy(0).start()
        for k in (1, 3, 2):
            kv_copy(k).start()
        prepare(q_ref, qdp, qda.at[0], 0)
        prepare(do_ref, qdp, qda.at[0], 1)
        for k in (1, 3, 2):
            qd_copy(k).start()
        red[...] = jnp.zeros_like(red)
        mixer_setup(me, raw_ref, bias_ref, rate_ref, doc_ref, drows, rows, tri, mk, vcol, small)
        group = hd // 2
        bf = group_cols(bin_ref, group)
        cf = group_cols(cout_ref, group)
        bg[...] = bf.astype(BF16)
        cg[...] = cf.astype(BF16)
        thr = rows[3][:, T - 1 : T]
        for e in range(NH):
            t = jnp.broadcast_to(thr[e : e + 1, :], (8, 128))
            hi = t.astype(BF16).astype(F32)
            pay[e, 64:80, :] = jnp.concatenate([hi, t - hi], axis=0).astype(BF16)
        pair_t[...] = dot(bf, cf, 1, 1, HI)
        doc = drows[pl.ds(RING + x_me, 1), :]
        dcol = col_of(doc, 128)
        dcol = jnp.concatenate([dcol, dcol], axis=1)
        bias_m[...] = jnp.where((tri[...] > 0.5) & (dcol == doc), 0.0, NEG)
        for ref in (dpair, dbt, dct, dcum, ddir, dskp, qs):
            ref[...] = jnp.zeros_like(ref)
        tail_copy.wait_recv()

    rows128 = pl.ds(pl.multiple_of(pair * 128, 128), 128)

    @pl.when(step_id < PAIRS)
    def _():
        x = conv_ref[...].astype(F32)
        pre = conv_forward(x, tail_rows(tail_in, pair), w_ref, mk, xs)
        act = pre * sigmoid(pre)
        gate = gate_ref[...].astype(F32)
        g = mix_ref[...].astype(F32) * (gate * sigmoid(gate))
        act_t = jnp.transpose(act)
        g_t = jnp.transpose(g)
        act_s[rows128, :] = act_t
        g_s[rows128, :] = g_t
        st = act_t * (pair_rows(rows, 0, pair) * pair_rows(rows, 4, pair))
        ge = g_t * pair_rows(rows, 3, pair)
        both = jnp.concatenate(
            [dot(st.astype(BF16), bg[...], 1, 0), dot(ge.astype(BF16), cg[...], 1, 0)], axis=1
        ).astype(BF16)
        pay[2 * pair, 0:64, :] = both[0:64]
        pay[2 * pair + 1, 0:64, :] = both[64:128]

    @pl.when(step_id == 7)
    def _():
        for k in (1, 3):
            kv_copy(k).wait_recv()
            halo_copy(k).start()

    @pl.when(step_id == PAIRS - 1)
    def _():
        kv_copy(2).wait_recv()
        halo_copy(2).start()

        def send_first(k, carry):
            peer = lax.rem(me + k, NSEQ)

            @pl.when(peer < NH)
            def _():
                first_copy(peer, me).start()

            return carry

        lax.fori_loop(1, NSEQ, send_first, 0)
        for k in range(1, RING):
            qd_copy(k).wait_recv()
        for k in range(RING):
            halo_copy(k).wait_recv()

        def send_dq(k):
            @pl.when(k > 0)
            def _():
                dq_copy(k).start()

        attention(x_me, kva, qda, drows, dka, dva, dq_out, send_dq)

        @pl.when(me < NH)
        def _():
            inbox[me] = pay[me]

            def wait_first(k, carry):
                first_copy(me, lax.rem(me + k, NSEQ)).wait_recv()
                return carry

            lax.fori_loop(1, NSEQ, wait_first, 0)
            lane = lax.broadcasted_iota(jnp.int32, (64, 128), 1)

            def gain(s):
                tail = inbox[s, 64:80, :].astype(F32)
                return tail[0:1] + tail[8:9]

            def down(s, run):
                outb[s] = run.astype(BF16)
                return gain(s) * run + inbox[s, 0:64, :].astype(F32)

            lax.fori_loop(0, NSEQ, down, jnp.zeros((64, 128), F32))

            def up(k, run):
                s = NSEQ - 1 - k
                outb[s] = jnp.where(lane < STATE, outb[s].astype(F32), run).astype(BF16)
                return gain(s) * run + inbox[s, 0:64, :].astype(F32)

            lax.fori_loop(0, NSEQ, up, jnp.zeros((64, 128), F32))

            def send_second(k, carry):
                second_copy(lax.rem(me + k, NSEQ), me).start()
                return carry

            lax.fori_loop(1, NSEQ, send_second, 0)
            landed[me] = outb[me]

        for k in range(RING):
            c = lax.rem(x_me + k, RING)
            back_out[k, 0] = (dka[c] * SCALE).astype(BF16)
            back_out[k, 1] = dva[c].astype(BF16)
            back_copy(k).start()
            own_out[k, 0] = (dka[RING + c] * SCALE).astype(BF16)
            own_out[k, 1] = dva[RING + c].astype(BF16)
            if k:
                own_copy(k).start()

    @pl.when(step_id == PAIRS)
    def _():
        def arrive(k, carry):
            peer = lax.rem(me + k, NSEQ)

            @pl.when(peer < NH)
            def _():
                second_copy(me, peer).wait_recv()

            return carry

        lax.fori_loop(1, NSEQ, arrive, 0)

    @pl.when(step_id >= PAIRS)
    def _():
        act_t = act_s[rows128, :]
        g_t = g_s[rows128, :]
        step_p = pair_rows(rows, 0, pair)
        eg_p = pair_rows(rows, 3, pair)
        te_p = pair_rows(rows, 4, pair)
        s_t = act_t * step_p
        s_b = s_t.astype(BF16)
        g_b = g_t.astype(BF16)
        state = jnp.concatenate([landed[2 * pair], landed[2 * pair + 1]], axis=0)
        start = state[:, 0:STATE]
        end = state[:, STATE:]
        car = dot(start, cg[...], 1, 1) * eg_p
        dste = dot(end, bg[...], 1, 1) * te_p
        dct[...] += dot(start, (g_t * eg_p).astype(BF16), 0, 0)
        dbt[...] += dot(end, (s_t * te_p).astype(BF16), 0, 0)
        se = start.astype(F32) * end.astype(F32)
        lane = lax.broadcasted_iota(jnp.int32, (1, T), 1)
        ys, dss = [], []
        for a in range(2):
            lo = 64 * a
            h = 2 * pair + a
            cum = rows[2, pl.ds(h, 1), :]
            cc = col_of(cum, 128)
            cc = jnp.concatenate([cc, cc], axis=1)
            w = jnp.exp(jnp.minimum(cum - cc, 0.0) + bias_m[...])
            m = pair_t[...] * w
            mb = m.astype(BF16)
            sh = s_b[lo : lo + 64]
            gh = g_b[lo : lo + 64]
            y = dot(sh, mb, 1, 0)
            dsi = dot(gh, mb, 1, 1)
            dm = dot(sh, gh, 0, 0)
            dpair[...] += dm * w
            z = dm * m
            zr = jnp.sum(jnp.transpose(z[:, 0:128] + z[:, 128:]), axis=0, keepdims=True)
            carh = car[lo : lo + 64]
            dsth = dste[lo : lo + 64]
            gt = g_t[lo : lo + 64]
            st = s_t[lo : lo + 64]
            at = act_t[lo : lo + 64]
            v = jnp.sum(st * dsth, axis=0, keepdims=True)
            d = jnp.sum(z, axis=0, keepdims=True) - zr + jnp.sum(gt * carh, axis=0, keepdims=True) - v
            thr = rows[3, pl.ds(h, 1), :][:, T - 1 : T]
            extra = jnp.sum(v, axis=1, keepdims=True) + thr * jnp.sum(
                jnp.sum(se[lo : lo + 64], axis=0, keepdims=True), axis=1, keepdims=True
            )
            dcum[pl.ds(h, 1), :] = d + jnp.where(lane == T - 1, extra, 0.0)
            ds = dsi + dsth
            ddir[pl.ds(h, 1), :] = jnp.sum(ds * at, axis=0, keepdims=True)
            dskp[pl.ds(h, 1), :] = jnp.sum(gt * at, axis=0, keepdims=True)
            skip = skip_ref[h]
            ys.append(y + carh + skip * at)
            dss.append(ds * step_p[lo : lo + 64] + skip * gt)
        y = jnp.transpose(jnp.concatenate(ys, axis=0))
        dact = jnp.transpose(jnp.concatenate(dss, axis=0))
        gate = gate_ref[...].astype(F32)
        sg = sigmoid(gate)
        dgate_out[...] = (
            mix_ref[...].astype(F32) * y * (sg * (1.0 + gate * (1.0 - sg)))
        ).astype(BF16)
        x = conv_ref[...].astype(F32)
        pre = conv_forward(x, tail_rows(tail_in, pair), w_ref, mk, xs)
        sp = sigmoid(pre)
        dpre = dact * (sp * (1.0 + pre * (1.0 - sp)))
        dx = None
        for k in range(4):
            q = dpre if k == 0 else dpre * mk[k - 1]
            red[pair, k : k + 1, :] = jnp.sum(q * xs[8 - k : 8 - k + T, :], axis=0, keepdims=True)
            qs[8 : 8 + T, :] = q
            term = w_ref[k : k + 1, :] * qs[k : k + 8 + T, :]
            dx = term if dx is None else dx + term
        spill[:, rows128] = dx[0:8]
        dconv_out[:, rows128] = dx[8:].astype(BF16)
        last[:, rows128] = dx[T - 8 :]

    @pl.when(step_id == 2 * PAIRS - 1)
    def _():
        dld = dot(dcum[...], tri[...], 1, 1, HI)
        rate = vcol[...]
        small[0:1, 0:NH] = bias_ref[...]
        bias = col_of(small[0:1, :], 128)[0:NH]
        v = raw_ref[...] + jnp.concatenate([bias, bias], axis=1)
        dldn = dld[0:NH]
        gs = (ddir[0:NH, :] - dldn * rate) * sigmoid(v)
        step_out[...] = gs
        pick = lax.broadcasted_iota(jnp.int32, (32, 128), 1)
        total = lambda z: jnp.sum(z, axis=1, keepdims=True)
        fscr[...] = jnp.zeros_like(fscr)
        fscr[0:NH, 0:128] = jnp.where(
            pick[0:NH] == 0,
            total(gs),
            jnp.where(pick[0:NH] == 1, total(dldn * rows[1, 0:NH, :]), total(dskp[0:NH, :])),
        )
        red[PAIRS] = jnp.transpose(fscr[0:128, 0:128])[0:8]
        dp = dpair[...].astype(BF16)
        coef_ref[0:STATE] = (dbt[...] + dot(jnp.transpose(cg[...].astype(F32)).astype(BF16), dp, 1, 1)).astype(BF16)
        coef_ref[STATE:] = (dct[...] + dot(jnp.transpose(bg[...].astype(F32)).astype(BF16), dp, 1, 0)).astype(BF16)

        def coef(k, frm):
            return pltpu.make_async_remote_copy(
                src_ref=coef_ref,
                dst_ref=cin.at[frm],
                send_sem=s3.at[k],
                recv_sem=r3.at[frm],
                device_id={"head": lax.rem(hd + k, 4)},
                device_id_type=MESH,
            )

        spill_copy = seq_copy(spill, spin, s4, r4, lax.rem(me + NSEQ - 1, NSEQ))

        def first(block, frm):
            return seq_copy(red.at[block], rinbox.at[frm], s1.at[block], r1.at[frm], 2 * block)

        def second(peer, block):
            return seq_copy(tot.at[block], tot.at[block], s2.at[peer], r2.at[block], peer)

        def send_first(b, carry):
            @pl.when(2 * b != me)
            def _():
                first(b, me).start()

            return carry

        lax.fori_loop(0, BLOCKS, send_first, 0)
        for k in range(1, 4):
            coef(k, hd).start()
        spill_copy.start()
        for k in range(RING):
            if k:
                dq_copy(k).wait_recv()
            h = lax.rem(x_me - k + RING, RING)
            source = dq_in if k else dq_out
            fscr[pl.ds(pl.multiple_of(h * HEAD_DIM, 32), HEAD_DIM), :] = source[k].astype(F32)
        gq_out[...] = jnp.transpose(fscr[...]).astype(BF16)
        mine = me // 2
        owner = (me == 2 * mine) & (mine < BLOCKS)

        @pl.when(owner)
        def _():
            rinbox[me] = red[mine]

            def wait_first(k, carry):
                first(mine, lax.rem(me + k, NSEQ)).wait_recv()
                return carry

            lax.fori_loop(1, NSEQ, wait_first, 0)
            tot[mine] = jnp.sum(rinbox[...], axis=0)

            def send_second(k, carry):
                second(lax.rem(me + k, NSEQ), mine).start()
                return carry

            lax.fori_loop(1, NSEQ, send_second, 0)

        for k in range(1, 4):
            coef(k, lax.rem(hd + k, 4)).wait_recv()
        cin[hd] = coef_ref[...]
        g0 = jnp.transpose(cin[0].astype(F32) + cin[1].astype(F32))
        g1 = jnp.transpose(cin[2].astype(F32) + cin[3].astype(F32))
        gin_out[...] = jnp.concatenate([g0[:, 0:STATE], g1[:, 0:STATE]], axis=1)
        gout_out[...] = jnp.concatenate([g0[:, STATE:], g1[:, STATE:]], axis=1)
        spill_copy.wait_recv()
        fixed = jnp.concatenate([last[0:8, :], last[8:16, :] + spin[...]], axis=0)
        dconv_out[T - 16 :, :] = fixed.astype(BF16)
        for k in range(RING):
            back_copy(k).wait_recv()
            if k:
                own_copy(k).wait_recv()
        for slot, dest in ((0, gk_out), (1, gv_out)):
            for k in range(RING):
                mine_k = own_in if k else own_out
                h = lax.rem(x_me - k + RING, RING)
                fscr[pl.ds(pl.multiple_of(h * HEAD_DIM, 32), HEAD_DIM), :] = mine_k[
                    k, slot
                ].astype(F32) + back_in[k, slot].astype(F32)
            dest[...] = jnp.transpose(fscr[...]).astype(BF16)

        def wait_second(b, carry):
            @pl.when(2 * b != me)
            def _():
                second(me, b).wait_recv()
                first(b, me).wait_send()

            return carry

        lax.fori_loop(0, BLOCKS, wait_second, 0)
        for p in range(PAIRS):
            dw_out[:, 128 * p : 128 * p + 128] = tot[p, 0:4, :]
        sc_out[...] = tot[PAIRS]

        @pl.when(owner)
        def _():
            def drain(k, carry):
                second(lax.rem(me + k, NSEQ), mine).wait_send()
                return carry

            lax.fori_loop(1, NSEQ, drain, 0)

        for k in range(1, 4):
            coef(k, hd).wait_send()
        spill_copy.wait_send()
        tail_copy.wait_send()
        for k in range(RING):
            halo_copy(k).wait_send()
            back_copy(k).wait_send()
            if k:
                kv_copy(k).wait_send()
                qd_copy(k).wait_send()
                dq_copy(k).wait_send()
                own_copy(k).wait_send()

        def sent_first(k, carry):
            peer = lax.rem(me + k, NSEQ)

            @pl.when(peer < NH)
            def _():
                first_copy(peer, me).wait_send()

            return carry

        lax.fori_loop(1, NSEQ, sent_first, 0)

        @pl.when(me < NH)
        def _():
            def sent_second(k, carry):
                second_copy(lax.rem(me + k, NSEQ), me).wait_send()
                return carry

            lax.fori_loop(1, NSEQ, sent_second, 0)


def whole_spec(shape):
    return pl.BlockSpec(shape, lambda i: (0,) * len(shape))


def layer(
    conv_input, gate_input, mix_grad, conv_weight, raw, bias, rate, docs, bin_, cout,
    queries, keys, values, attn_grad, skip,
):
    tok = pl.BlockSpec((T, 128), lambda i: (0, lax.rem(i, PAIRS)))
    piece = jax.ShapeDtypeStruct((T, 4 * HEAD_DIM), BF16)
    outs = [
        jax.ShapeDtypeStruct((T, WIDTH), BF16),
        jax.ShapeDtypeStruct((T, WIDTH), BF16),
        jax.ShapeDtypeStruct((NH, T), F32),
        jax.ShapeDtypeStruct((4, WIDTH), F32),
        jax.ShapeDtypeStruct((8, 128), F32),
        jax.ShapeDtypeStruct((T, 128), F32),
        jax.ShapeDtypeStruct((T, 128), F32),
        piece,
        piece,
        piece,
    ]
    specs = [whole_spec(o.shape) for o in outs]
    specs[1] = pl.BlockSpec((T, 128), lambda i: (0, jnp.maximum(i - PAIRS, 0)))
    square = VM((T, T), F32)
    heads = VM((32, T), F32)
    return pl.pallas_call(
        layer_kernel,
        grid=(2 * PAIRS,),
        in_specs=[
            tok,
            tok,
            tok,
            pl.BlockSpec((4, 128), lambda i: (0, lax.rem(i, PAIRS))),
            whole_spec((NH, T)),
            whole_spec((1, NH)),
            whole_spec((1, NH)),
            whole_spec((64, 128)),
            whole_spec((T, 128)),
            whole_spec((T, 128)),
        ]
        + [whole_spec((T, 4 * HEAD_DIM))] * 4
        + [
            pl.BlockSpec((16, WIDTH), lambda i: (T // 16 - 1, 0)),
            pl.BlockSpec(memory_space=pltpu.SMEM),
        ],
        out_specs=specs,
        out_shape=outs,
        scratch_shapes=[
            VM((8, T), F32),
            VM((5, 32, T), F32),
            square,
            VM((3, T, 128), F32),
            VM((NH, T), F32),
            VM((8, 128), F32),
            VM((8 + T, 128), F32),
            VM((T, STATE), BF16),
            VM((T, STATE), BF16),
            VM((WIDTH, T), F32),
            VM((WIDTH, T), F32),
            VM((RING, 2, HEAD_DIM, T), BF16),
            VM((RING, 2, HEAD_DIM, T), BF16),
            VM((4 * HEAD_DIM, T), BF16),
            VM((2 * RING, 2, HEAD_DIM, T), BF16),
            VM((RING, 2, HEAD_DIM, T), BF16),
            VM((16, WIDTH), BF16),
            VM((NH, 80, 128), BF16),
            VM((NSEQ, 80, 128), BF16),
            VM((NSEQ, 64, 128), BF16),
            VM((NH, 64, 128), BF16),
            VM((2 * RING, HEAD_DIM, T), F32),
            VM((2 * RING, HEAD_DIM, T), F32),
            VM((RING, HEAD_DIM, T), BF16),
            VM((RING, 2, HEAD_DIM, T), BF16),
            VM((RING, 2, HEAD_DIM, T), BF16),
            VM((RING, HEAD_DIM, T), BF16),
            VM((RING, 2, HEAD_DIM, T), BF16),
            VM((RING, 2, HEAD_DIM, T), BF16),
            VM((4 * HEAD_DIM, T), F32),
            square,
            square,
            square,
            heads,
            heads,
            heads,
            VM((STATE, T), F32),
            VM((STATE, T), F32),
            VM((16 + T, 128), F32),
            VM((16, WIDTH), F32),
            VM((8, WIDTH), F32),
            VM((8, WIDTH), F32),
            VM((BLOCKS, 8, 128), F32),
            VM((NSEQ, 8, 128), F32),
            VM((BLOCKS, 8, 128), F32),
            VM((128, T), BF16),
            VM((4, 128, T), BF16),
            DMA((RING,)), DMA((RING,)), DMA((RING,)), DMA((RING,)), DMA((RING,)), DMA((RING,)),
            DMA, DMA,
            DMA((NSEQ,)), DMA((NSEQ,)), DMA((NSEQ,)), DMA((NSEQ,)),
            DMA((RING,)), DMA((RING,)), DMA((RING,)), DMA((RING,)), DMA((RING,)), DMA((RING,)),
            DMA((BLOCKS,)), DMA((NSEQ,)), DMA((NSEQ,)), DMA((BLOCKS,)),
            DMA((4,)), DMA((4,)), DMA, DMA,
        ],
        compiler_params=pltpu.CompilerParams(
            collective_id=1, has_side_effects=True, vmem_limit_bytes=60 * 1024 * 1024
        ),
        name="layer",
        cost_estimate=pl.CostEstimate(
            flops=6000000000, bytes_accessed=12000000, transcendentals=6000000
        ),
    )(
        conv_input, gate_input, mix_grad, conv_weight, raw, bias, rate, docs, bin_, cout,
        queries, keys, values, attn_grad, conv_input, skip,
    )


def finish_kernel(*refs):
    half = len(refs) // 2
    for src, dest in zip(refs[:half], refs[half:]):
        dest[...] = src[...]


def finish(arrays):
    parts = 7

    def spec(a):
        if a.shape[0] == T and a.shape[1] > 128:
            return pl.BlockSpec((T, a.shape[1] // parts), lambda i: (0, i))
        return whole_spec(a.shape)

    specs = [spec(a) for a in arrays]
    return pl.pallas_call(
        finish_kernel,
        grid=(parts,),
        in_specs=specs,
        out_specs=specs,
        out_shape=[jax.ShapeDtypeStruct(a.shape, a.dtype) for a in arrays],
        compiler_params=pltpu.CompilerParams(vmem_limit_bytes=60 * 1024 * 1024),
        name="finish",
        cost_estimate=pl.CostEstimate(flops=1000000, bytes_accessed=7000000, transcendentals=0),
    )(*arrays)


def local(
    queries, keys, values, attn_grad, doc_ids, conv_input, conv_weight, step_raw, step_bias,
    rate_log, skip_gain, input_coeff, output_coeff, gate_input, mix_grad,
):
    outs = layer(
        conv_input, gate_input, mix_grad, conv_weight, step_raw.T, step_bias[None],
        rate_log[None], doc_ids.reshape(64, 128), input_coeff, output_coeff, queries, keys,
        values, attn_grad, skip_gain,
    )
    dconv, dgate, gstep, dw, sc, gin, gout, gq, gk, gv = finish(outs)
    return (
        gq, gk, gv, dconv, dgate, gstep.T, gin, gout, dw, sc[0, :NH], sc[1, :NH], sc[2, :NH]
    )


def solution(mesh):
    both = P("seq", "head")
    return jax.shard_map(
        local,
        mesh=mesh,
        in_specs=(
            both, both, both, both, P(), both, P(None, "head"), both, P("head"), P("head"),
            P("head"), P("seq", None), P("seq", None), both, both,
        ),
        out_specs=(
            both, both, both, both, both, both, P("seq", None), P("seq", None),
            P(None, "head"), P("head"), P("head"), P("head"),
        ),
        check_vma=False,
    )
```

```python
import jax
import jax.numpy as jnp
from jax import lax
from jax.experimental import pallas as pl
from jax.experimental.pallas import tpu as pltpu
from jax.sharding import PartitionSpec as P

HEAD_DIM = 224
WINDOW = 1024
SSM_HEADS = 112
STATE = 64
GROUPS = 2
T = 256
NH = 28
PAIRS = 14
NSEQ = 32
RING = 4
NEG = -1e30
F32 = jnp.float32
BF16 = jnp.bfloat16
MESH = pl.DeviceIdType.MESH
VM = pltpu.VMEM
SCALE = HEAD_DIM ** (-0.5)
HI = lax.Precision.HIGHEST


def dot(a, b, ca, cb, precision=None):
    return lax.dot_general(
        a, b, (((ca,), (cb,)), ((), ())), preferred_element_type=F32, precision=precision
    )


def sigmoid(v):
    return 1.0 / (1.0 + jnp.exp(-v))


def col_of(row, rows):
    return jnp.transpose(jnp.broadcast_to(row, (rows, row.shape[1])))


DMA = pltpu.SemaphoreType.DMA
WIDTH = NH * 64
BLOCKS = PAIRS + 1
ANY = pl.BlockSpec(memory_space=pl.ANY)


def doc_row(ref, shard):
    safe = jnp.maximum(shard, 0) * 2
    row = jnp.concatenate([ref[pl.ds(safe, 1), :], ref[pl.ds(safe + 1, 1), :]], axis=1)
    return jnp.where(shard < 0, -1.0, row.astype(F32))


def mixer_setup(me, raw_ref, bias_ref, rate_ref, doc_ref, drows, rows, tri, mk, vcol, small):
    base = me - lax.rem(me, RING)
    for c in range(2 * RING):
        drows[c : c + 1, :] = doc_row(doc_ref, base - RING + c)
    doc = doc_row(doc_ref, me)
    prev = doc_row(doc_ref, me - 1)
    small[...] = jnp.zeros_like(small)
    small[0:1, 0:NH] = bias_ref[...]
    small[1:2, 0:NH] = jnp.exp(rate_ref[...])
    bias = col_of(small[0:1, :], 128)[0:NH]
    rate = col_of(small[1:2, :], 128)[0:NH]
    vcol[...] = jnp.concatenate([rate, rate], axis=1)
    rows[...] = jnp.zeros_like(rows)
    step = jnp.log(1.0 + jnp.exp(raw_ref[...] + jnp.concatenate([bias, bias], axis=1)))
    rows[0, 0:NH, :] = step
    rows[1, 0:NH, :] = -step * vcol[...]
    i = lax.broadcasted_iota(jnp.int32, (T, T), 0)
    j = lax.broadcasted_iota(jnp.int32, (T, T), 1)
    tri[...] = jnp.where(i <= j, 1.0, 0.0)
    cum = dot(rows[1], tri[...], 1, 0, HI)
    rows[2] = cum
    rows[3] = jnp.where(doc == prev[:, T - 1 : T], jnp.exp(cum), 0.0)
    rows[4] = jnp.where(
        doc == doc[:, T - 1 : T], jnp.exp(jnp.minimum(cum[:, T - 1 : T] - cum, 0.0)), 0.0
    )
    lane = lax.broadcasted_iota(jnp.int32, (8, T), 1)
    doc8 = jnp.broadcast_to(doc, (8, T))
    prev8 = jnp.broadcast_to(prev, (8, T))
    for k in range(1, 4):
        lag = jnp.where(lane < k, pltpu.roll(prev8, k, 1), pltpu.roll(doc8, k, 1))
        mk[k - 1] = col_of(jnp.where(lag == doc8, 1.0, 0.0)[0:1, :], 128)


def pair_rows(rows, which, pair):
    a = rows[which, pl.ds(2 * pair, 1), :]
    b = rows[which, pl.ds(2 * pair + 1, 1), :]
    return jnp.concatenate(
        [jnp.broadcast_to(a, (64, T)), jnp.broadcast_to(b, (64, T))], axis=0
    )


def group_cols(ref, group):
    v = ref[...].astype(F32)
    return jnp.where(group == 0, v[:, 0:STATE], v[:, STATE:])


def conv_forward(x, tail, w_ref, mk, xs):
    xs[0:8, :] = tail
    xs[8 : 8 + T, :] = x
    pre = w_ref[0:1, :] * x
    for k in range(1, 4):
        pre = pre + w_ref[k : k + 1, :] * (mk[k - 1] * xs[8 - k : 8 - k + T, :])
    return pre


def tail_rows(ref, pair):
    lanes = pl.ds(pl.multiple_of(pair * 128, 128), 128)
    return ref[:, lanes].astype(F32)[8:16]


def seq_copy(src, dst, send, recv, peer):
    return pltpu.make_async_remote_copy(
        src_ref=src,
        dst_ref=dst,
        send_sem=send,
        recv_sem=recv,
        device_id={"seq": peer},
        device_id_type=MESH,
    )


def greet_seq(barrier, me):
    def greet(k, carry):
        peer = lax.rem(me + k, NSEQ)
        pl.semaphore_signal(barrier, inc=1, device_id={"seq": peer}, device_id_type=MESH)
        return carry

    lax.fori_loop(1, NSEQ, greet, 0)


def attention(x_me, kva, qda, drows, dka, dva, dq_out, send_dq, midway):
    dka[...] = jnp.zeros_like(dka)
    dva[...] = jnp.zeros_like(dva)
    row_i = lax.broadcasted_iota(jnp.int32, (T, T), 0)
    col_j = lax.broadcasted_iota(jnp.int32, (T, T), 1)

    def chunk(c, carry):
        pl.when(c == 2)(midway)
        slot = lax.rem(x_me - c + RING, RING)
        qt = qda[slot, 0]
        gt = qda[slot, 1]
        q = jnp.transpose(qt.astype(F32)).astype(BF16)
        g = jnp.transpose(gt.astype(F32)).astype(BF16)
        dq_col = col_of(drows[pl.ds(RING + c, 1), :], 128)
        dq_col = jnp.concatenate([dq_col, dq_col], axis=1)
        scores, masks, slots = [], [], []
        row_max = None
        for b in range(RING + 1):
            kc = c + b
            slots.append(kc // RING * RING + lax.rem(x_me - kc + 2 * RING, RING))
            s = dot(q, kva[slots[b], 0], 1, 0) * SCALE
            ok = dq_col == drows[pl.ds(kc, 1), :]
            if b == 0:
                ok = ok & (col_j > row_i)
            if b == RING:
                ok = ok & (col_j <= row_i)
            s = jnp.where(ok, s, NEG)
            scores.append(s)
            masks.append(ok)
            m = jnp.max(s, axis=1, keepdims=True)
            row_max = m if row_max is None else jnp.maximum(row_max, m)
        row_sum = None
        for b in range(RING + 1):
            e = jnp.where(masks[b], jnp.exp(scores[b] - row_max), 0.0)
            scores[b] = e
            r = jnp.sum(e, axis=1, keepdims=True)
            row_sum = r if row_sum is None else row_sum + r
        inv = 1.0 / jnp.maximum(row_sum, 1.0)
        dprobs = []
        delta = None
        for b in range(RING + 1):
            p = scores[b] * inv
            scores[b] = p
            half = p.astype(BF16)
            dp = dot(g, kva[slots[b], 1], 1, 0)
            dprobs.append(dp)
            r = jnp.sum(half.astype(F32) * dp, axis=1, keepdims=True)
            delta = r if delta is None else delta + r
            dva[c + b] = dva[c + b] + dot(gt, half, 1, 0)
        dqt = None
        for b in range(RING + 1):
            ds = (scores[b] * (dprobs[b] - delta)).astype(BF16)
            r = dot(kva[slots[b], 0], ds, 1, 1)
            dqt = r if dqt is None else dqt + r
            dka[c + b] = dka[c + b] + dot(qt, ds, 1, 0)
        k = lax.rem(c - x_me + RING, RING)
        dq_out[k] = (dqt * SCALE).astype(BF16)
        send_dq(k)
        return carry

    lax.fori_loop(0, RING, chunk, 0)


def layer_kernel(
    conv_ref, gate_ref, mix_ref, w_ref, raw_ref, bias_ref, rate_ref, doc_ref, bin_ref, cout_ref,
    q_ref, k_ref, v_ref, do_ref, edge_ref, skip_ref,
    dconv_out, dgate_out, step_out, dw_out, sc_out, gin_out, gout_out, gq_out, gk_out, gv_out,
    drows, rows, tri, mk, vcol, small, xs, bg, cg, act_s, g_s, y_s, ds_s,
    kvp, qdp, tscr, kva, qda, tail_in, pay, inbox, outb, landed,
    dka, dva, dq_out, own_out, back_out, dq_in, own_in, back_in, fscr,
    bias_m, pair_t, dpair, dcum, ddir, dskp, dbt, dct, qs,
    last, spill, spin, red, rinbox, tot, coef_ref, cin,
    hs, hr, ks, kr, qsm, qr, ts, tr, cs1, cr1, cs2, cr2,
    ds_, dr, osm, orr, bs, br, s1, r1, s2, r2, s3, r3, s4, r4,
):
    step_id = pl.program_id(0)
    pair = lax.rem(step_id, PAIRS)
    me = lax.axis_index("seq")
    hd = lax.axis_index("head")
    x_me = lax.rem(me, RING)
    base = me - x_me
    fwd = lax.rem(base + RING, NSEQ)
    bwd = lax.rem(base + NSEQ - RING, NSEQ)

    def near(k):
        return base + lax.rem(x_me + k, RING)

    def halo_copy(k):
        return seq_copy(kva.at[RING + k], kva.at[k], hs.at[k], hr.at[k], fwd + x_me)

    def kv_copy(k):
        return seq_copy(kvp.at[k], kva.at[RING + k], ks.at[k], kr.at[k], near(k))

    def qd_copy(k):
        return seq_copy(qdp.at[k], qda.at[k], qsm.at[k], qr.at[k], near(k))

    def dq_copy(k):
        return seq_copy(dq_out.at[k], dq_in.at[k], ds_.at[k], dr.at[k], near(k))

    def own_copy(k):
        return seq_copy(own_out.at[k], own_in.at[k], osm.at[k], orr.at[k], near(k))

    def back_copy(k):
        return seq_copy(
            back_out.at[k], back_in.at[k], bs.at[k], br.at[k], bwd + lax.rem(x_me + k, RING)
        )

    def first_copy(peer, frm):
        return seq_copy(pay.at[peer], inbox.at[frm], cs1.at[peer], cr1.at[frm], peer)

    def second_copy(peer, frm):
        return seq_copy(outb.at[peer], landed.at[frm], cs2.at[peer], cr2.at[frm], peer)

    tail_copy = seq_copy(edge_ref, tail_in, ts, tr, lax.rem(me + 1, NSEQ))

    @pl.when(step_id == 0)
    def _():
        barrier = pltpu.get_barrier_semaphore()
        greet_seq(barrier, me)
        for k in range(1, 4):
            pl.semaphore_signal(
                barrier, inc=1, device_id={"head": lax.rem(hd + k, 4)}, device_id_type=MESH
            )

        def prepare(src, dest, landing, slot):
            tscr[...] = jnp.transpose(src[...].astype(F32)).astype(BF16)
            for k in range(RING):
                h = lax.rem(x_me + k, RING)
                part = tscr[pl.ds(pl.multiple_of(h * HEAD_DIM, 32), HEAD_DIM), :]
                if k:
                    dest[k, slot] = part
                else:
                    landing[slot] = part

        prepare(k_ref, kvp, kva.at[RING], 0)
        prepare(v_ref, kvp, kva.at[RING], 1)
        pl.semaphore_wait(barrier, NSEQ + 2)
        tail_copy.start()
        halo_copy(0).start()
        for k in (1, 3, 2):
            kv_copy(k).start()
        prepare(q_ref, qdp, qda.at[0], 0)
        prepare(do_ref, qdp, qda.at[0], 1)
        for k in (1, 3, 2):
            qd_copy(k).start()
        red[...] = jnp.zeros_like(red)
        mixer_setup(me, raw_ref, bias_ref, rate_ref, doc_ref, drows, rows, tri, mk, vcol, small)
        group = hd // 2
        bf = group_cols(bin_ref, group)
        cf = group_cols(cout_ref, group)
        bg[...] = bf.astype(BF16)
        cg[...] = cf.astype(BF16)
        thr = rows[3][:, T - 1 : T]
        for e in range(NH):
            t = jnp.broadcast_to(thr[e : e + 1, :], (8, 128))
            hi = t.astype(BF16).astype(F32)
            pay[e, 64:80, :] = jnp.concatenate([hi, t - hi], axis=0).astype(BF16)
        pair_t[...] = dot(bf, cf, 1, 1, HI)
        doc = drows[pl.ds(RING + x_me, 1), :]
        dcol = col_of(doc, 128)
        dcol = jnp.concatenate([dcol, dcol], axis=1)
        bias_m[...] = jnp.where((tri[...] > 0.5) & (dcol == doc), 0.0, NEG)
        for ref in (dpair, dbt, dct, dcum, ddir, dskp, qs):
            ref[...] = jnp.zeros_like(ref)
        tail_copy.wait_recv()

    rows128 = pl.ds(pl.multiple_of(pair * 128, 128), 128)

    @pl.when(step_id < PAIRS)
    def _():
        x = conv_ref[...].astype(F32)
        pre = conv_forward(x, tail_rows(tail_in, pair), w_ref, mk, xs)
        act = pre * sigmoid(pre)
        gate = gate_ref[...].astype(F32)
        g = mix_ref[...].astype(F32) * (gate * sigmoid(gate))
        act_t = jnp.transpose(act)
        g_t = jnp.transpose(g)
        act_s[rows128, :] = act_t
        g_s[rows128, :] = g_t
        st = act_t * (pair_rows(rows, 0, pair) * pair_rows(rows, 4, pair))
        ge = g_t * pair_rows(rows, 3, pair)
        both = jnp.concatenate(
            [dot(st.astype(BF16), bg[...], 1, 0), dot(ge.astype(BF16), cg[...], 1, 0)], axis=1
        ).astype(BF16)
        pay[2 * pair, 0:64, :] = both[0:64]
        pay[2 * pair + 1, 0:64, :] = both[64:128]

    @pl.when(step_id == 7)
    def _():
        for k in (1, 3):
            kv_copy(k).wait_recv()
            halo_copy(k).start()

    @pl.when(step_id == PAIRS - 1)
    def _():
        kv_copy(2).wait_recv()
        halo_copy(2).start()

        def send_first(k, carry):
            peer = lax.rem(me + k, NSEQ)

            @pl.when(peer < NH)
            def _():
                first_copy(peer, me).start()

            return carry

        lax.fori_loop(1, NSEQ, send_first, 0)

    @pl.when(step_id == 2 * PAIRS - 1)
    def _():
        for k in range(1, RING):
            qd_copy(k).wait_recv()
        for k in range(RING):
            halo_copy(k).wait_recv()

        def send_dq(k):
            @pl.when(k > 0)
            def _():
                dq_copy(k).start()

        def midway():
            @pl.when(me < NH)
            def _():
                inbox[me] = pay[me]

                def wait_first(k, carry):
                    first_copy(me, lax.rem(me + k, NSEQ)).wait_recv()
                    return carry

                lax.fori_loop(1, NSEQ, wait_first, 0)
                lane = lax.broadcasted_iota(jnp.int32, (64, 128), 1)

                def gain(s):
                    tail = inbox[s, 64:80, :].astype(F32)
                    return tail[0:1] + tail[8:9]

                def down(s, run):
                    outb[s] = run.astype(BF16)
                    return gain(s) * run + inbox[s, 0:64, :].astype(F32)

                lax.fori_loop(0, NSEQ, down, jnp.zeros((64, 128), F32))

                def up(k, run):
                    s = NSEQ - 1 - k
                    outb[s] = jnp.where(lane < STATE, outb[s].astype(F32), run).astype(BF16)
                    return gain(s) * run + inbox[s, 0:64, :].astype(F32)

                lax.fori_loop(0, NSEQ, up, jnp.zeros((64, 128), F32))

                def send_second(k, carry):
                    second_copy(lax.rem(me + k, NSEQ), me).start()
                    return carry

                lax.fori_loop(1, NSEQ, send_second, 0)
                landed[me] = outb[me]

        attention(x_me, kva, qda, drows, dka, dva, dq_out, send_dq, midway)
        for k in range(RING):
            c = lax.rem(x_me + k, RING)
            back_out[k, 0] = (dka[c] * SCALE).astype(BF16)
            back_out[k, 1] = dva[c].astype(BF16)
            back_copy(k).start()
            own_out[k, 0] = (dka[RING + c] * SCALE).astype(BF16)
            own_out[k, 1] = dva[RING + c].astype(BF16)
            if k:
                own_copy(k).start()

    @pl.when(step_id == 2 * PAIRS)
    def _():
        def arrive(k, carry):
            peer = lax.rem(me + k, NSEQ)

            @pl.when(peer < NH)
            def _():
                second_copy(me, peer).wait_recv()

            return carry

        lax.fori_loop(1, NSEQ, arrive, 0)

    @pl.when((step_id >= PAIRS) & (step_id < 2 * PAIRS))
    def _():
        act_t = act_s[rows128, :]
        g_t = g_s[rows128, :]
        s_b = (act_t * pair_rows(rows, 0, pair)).astype(BF16)
        g_b = g_t.astype(BF16)
        ys, dss = [], []
        for a in range(2):
            lo = 64 * a
            h = 2 * pair + a
            cum = rows[2, pl.ds(h, 1), :]
            cc = col_of(cum, 128)
            cc = jnp.concatenate([cc, cc], axis=1)
            w = jnp.exp(jnp.minimum(cum - cc, 0.0) + bias_m[...])
            m = pair_t[...] * w
            mb = m.astype(BF16)
            sh = s_b[lo : lo + 64]
            gh = g_b[lo : lo + 64]
            ys.append(dot(sh, mb, 1, 0))
            dsi = dot(gh, mb, 1, 1)
            dss.append(dsi)
            dm = dot(sh, gh, 0, 0)
            dpair[...] += dm * w
            z = dm * m
            zr = jnp.sum(jnp.transpose(z[:, 0:128] + z[:, 128:]), axis=0, keepdims=True)
            at = act_t[lo : lo + 64]
            dcum[pl.ds(h, 1), :] = jnp.sum(z, axis=0, keepdims=True) - zr
            ddir[pl.ds(h, 1), :] = jnp.sum(dsi * at, axis=0, keepdims=True)
            dskp[pl.ds(h, 1), :] = jnp.sum(g_t[lo : lo + 64] * at, axis=0, keepdims=True)
        y_s[rows128, :] = jnp.concatenate(ys, axis=0)
        ds_s[rows128, :] = jnp.concatenate(dss, axis=0)

    @pl.when(step_id >= 2 * PAIRS)
    def _():
        act_t = act_s[rows128, :]
        g_t = g_s[rows128, :]
        step_p = pair_rows(rows, 0, pair)
        eg_p = pair_rows(rows, 3, pair)
        te_p = pair_rows(rows, 4, pair)
        s_t = act_t * step_p
        state = jnp.concatenate([landed[2 * pair], landed[2 * pair + 1]], axis=0)
        start = state[:, 0:STATE]
        end = state[:, STATE:]
        car = dot(start, cg[...], 1, 1) * eg_p
        dste = dot(end, bg[...], 1, 1) * te_p
        dct[...] += dot(start, (g_t * eg_p).astype(BF16), 0, 0)
        dbt[...] += dot(end, (s_t * te_p).astype(BF16), 0, 0)
        se = start.astype(F32) * end.astype(F32)
        lane = lax.broadcasted_iota(jnp.int32, (1, T), 1)
        skips = []
        for a in range(2):
            part = slice(64 * a, 64 * a + 64)
            h = 2 * pair + a
            v = jnp.sum(s_t[part] * dste[part], axis=0, keepdims=True)
            d = jnp.sum(g_t[part] * car[part], axis=0, keepdims=True) - v
            thr = rows[3, pl.ds(h, 1), :][:, T - 1 : T]
            extra = jnp.sum(v, axis=1, keepdims=True) + thr * jnp.sum(
                jnp.sum(se[part], axis=0, keepdims=True), axis=1, keepdims=True
            )
            dcum[pl.ds(h, 1), :] += d + jnp.where(lane == T - 1, extra, 0.0)
            ddir[pl.ds(h, 1), :] += jnp.sum(dste[part] * act_t[part], axis=0, keepdims=True)
            skips.append(jnp.full((64, T), skip_ref[h], F32))
        skip = jnp.concatenate(skips, axis=0)
        y = jnp.transpose(y_s[rows128, :] + car + skip * act_t)
        dact = jnp.transpose((ds_s[rows128, :] + dste) * step_p + skip * g_t)
        gate = gate_ref[...].astype(F32)
        sg = sigmoid(gate)
        dgate_out[...] = (
            mix_ref[...].astype(F32) * y * (sg * (1.0 + gate * (1.0 - sg)))
        ).astype(BF16)
        x = conv_ref[...].astype(F32)
        pre = conv_forward(x, tail_rows(tail_in, pair), w_ref, mk, xs)
        sp = sigmoid(pre)
        dpre = dact * (sp * (1.0 + pre * (1.0 - sp)))
        dx = None
        for k in range(4):
            q = dpre if k == 0 else dpre * mk[k - 1]
            red[pair, k : k + 1, :] = jnp.sum(q * xs[8 - k : 8 - k + T, :], axis=0, keepdims=True)
            qs[8 : 8 + T, :] = q
            term = w_ref[k : k + 1, :] * qs[k : k + 8 + T, :]
            dx = term if dx is None else dx + term
        spill[:, rows128] = dx[0:8]
        dconv_out[:, rows128] = dx[8:].astype(BF16)
        last[:, rows128] = dx[T - 8 :]

    @pl.when(step_id == 3 * PAIRS - 1)
    def _():
        dld = dot(dcum[...], tri[...], 1, 1, HI)
        rate = vcol[...]
        small[0:1, 0:NH] = bias_ref[...]
        bias = col_of(small[0:1, :], 128)[0:NH]
        v = raw_ref[...] + jnp.concatenate([bias, bias], axis=1)
        dldn = dld[0:NH]
        gs = (ddir[0:NH, :] - dldn * rate) * sigmoid(v)
        step_out[...] = gs
        pick = lax.broadcasted_iota(jnp.int32, (32, 128), 1)
        total = lambda z: jnp.sum(z, axis=1, keepdims=True)
        fscr[...] = jnp.zeros_like(fscr)
        fscr[0:NH, 0:128] = jnp.where(
            pick[0:NH] == 0,
            total(gs),
            jnp.where(pick[0:NH] == 1, total(dldn * rows[1, 0:NH, :]), total(dskp[0:NH, :])),
        )
        red[PAIRS] = jnp.transpose(fscr[0:128, 0:128])[0:8]
        dp = dpair[...].astype(BF16)
        coef_ref[0:STATE] = (dbt[...] + dot(jnp.transpose(cg[...].astype(F32)).astype(BF16), dp, 1, 1)).astype(BF16)
        coef_ref[STATE:] = (dct[...] + dot(jnp.transpose(bg[...].astype(F32)).astype(BF16), dp, 1, 0)).astype(BF16)

        def coef(k, frm):
            return pltpu.make_async_remote_copy(
                src_ref=coef_ref,
                dst_ref=cin.at[frm],
                send_sem=s3.at[k],
                recv_sem=r3.at[frm],
                device_id={"head": lax.rem(hd + k, 4)},
                device_id_type=MESH,
            )

        spill_copy = seq_copy(spill, spin, s4, r4, lax.rem(me + NSEQ - 1, NSEQ))

        def first(block, frm):
            return seq_copy(red.at[block], rinbox.at[frm], s1.at[block], r1.at[frm], 2 * block)

        def second(peer, block):
            return seq_copy(tot.at[block], tot.at[block], s2.at[peer], r2.at[block], peer)

        def send_first(b, carry):
            @pl.when(2 * b != me)
            def _():
                first(b, me).start()

            return carry

        lax.fori_loop(0, BLOCKS, send_first, 0)
        for k in range(1, 4):
            coef(k, hd).start()
        spill_copy.start()
        for k in range(RING):
            if k:
                dq_copy(k).wait_recv()
            h = lax.rem(x_me - k + RING, RING)
            source = dq_in if k else dq_out
            fscr[pl.ds(pl.multiple_of(h * HEAD_DIM, 32), HEAD_DIM), :] = source[k].astype(F32)
        gq_out[...] = jnp.transpose(fscr[...]).astype(BF16)
        mine = me // 2
        owner = (me == 2 * mine) & (mine < BLOCKS)

        @pl.when(owner)
        def _():
            rinbox[me] = red[mine]

            def wait_first(k, carry):
                first(mine, lax.rem(me + k, NSEQ)).wait_recv()
                return carry

            lax.fori_loop(1, NSEQ, wait_first, 0)
            tot[mine] = jnp.sum(rinbox[...], axis=0)

            def send_second(k, carry):
                second(lax.rem(me + k, NSEQ), mine).start()
                return carry

            lax.fori_loop(1, NSEQ, send_second, 0)

        for k in range(1, 4):
            coef(k, lax.rem(hd + k, 4)).wait_recv()
        cin[hd] = coef_ref[...]
        g0 = jnp.transpose(cin[0].astype(F32) + cin[1].astype(F32))
        g1 = jnp.transpose(cin[2].astype(F32) + cin[3].astype(F32))
        gin_out[...] = jnp.concatenate([g0[:, 0:STATE], g1[:, 0:STATE]], axis=1)
        gout_out[...] = jnp.concatenate([g0[:, STATE:], g1[:, STATE:]], axis=1)
        spill_copy.wait_recv()
        fixed = jnp.concatenate([last[0:8, :], last[8:16, :] + spin[...]], axis=0)
        dconv_out[T - 16 :, :] = fixed.astype(BF16)
        for k in range(RING):
            back_copy(k).wait_recv()
            if k:
                own_copy(k).wait_recv()
        for slot, dest in ((0, gk_out), (1, gv_out)):
            for k in range(RING):
                mine_k = own_in if k else own_out
                h = lax.rem(x_me - k + RING, RING)
                fscr[pl.ds(pl.multiple_of(h * HEAD_DIM, 32), HEAD_DIM), :] = mine_k[
                    k, slot
                ].astype(F32) + back_in[k, slot].astype(F32)
            dest[...] = jnp.transpose(fscr[...]).astype(BF16)

        def wait_second(b, carry):
            @pl.when(2 * b != me)
            def _():
                second(me, b).wait_recv()
                first(b, me).wait_send()

            return carry

        lax.fori_loop(0, BLOCKS, wait_second, 0)
        for p in range(PAIRS):
            dw_out[:, 128 * p : 128 * p + 128] = tot[p, 0:4, :]
        sc_out[...] = tot[PAIRS]

        @pl.when(owner)
        def _():
            def drain(k, carry):
                second(lax.rem(me + k, NSEQ), mine).wait_send()
                return carry

            lax.fori_loop(1, NSEQ, drain, 0)

        for k in range(1, 4):
            coef(k, hd).wait_send()
        spill_copy.wait_send()
        tail_copy.wait_send()
        for k in range(RING):
            halo_copy(k).wait_send()
            back_copy(k).wait_send()
            if k:
                kv_copy(k).wait_send()
                qd_copy(k).wait_send()
                dq_copy(k).wait_send()
                own_copy(k).wait_send()

        def sent_first(k, carry):
            peer = lax.rem(me + k, NSEQ)

            @pl.when(peer < NH)
            def _():
                first_copy(peer, me).wait_send()

            return carry

        lax.fori_loop(1, NSEQ, sent_first, 0)

        @pl.when(me < NH)
        def _():
            def sent_second(k, carry):
                second_copy(lax.rem(me + k, NSEQ), me).wait_send()
                return carry

            lax.fori_loop(1, NSEQ, sent_second, 0)


def whole_spec(shape):
    return pl.BlockSpec(shape, lambda i: (0,) * len(shape))


def layer(
    conv_input, gate_input, mix_grad, conv_weight, raw, bias, rate, docs, bin_, cout,
    queries, keys, values, attn_grad, skip,
):
    tok = pl.BlockSpec((T, 128), lambda i: (0, lax.rem(i, PAIRS)))
    piece = jax.ShapeDtypeStruct((T, 4 * HEAD_DIM), BF16)
    outs = [
        jax.ShapeDtypeStruct((T, WIDTH), BF16),
        jax.ShapeDtypeStruct((T, WIDTH), BF16),
        jax.ShapeDtypeStruct((NH, T), F32),
        jax.ShapeDtypeStruct((4, WIDTH), F32),
        jax.ShapeDtypeStruct((8, 128), F32),
        jax.ShapeDtypeStruct((T, 128), F32),
        jax.ShapeDtypeStruct((T, 128), F32),
        piece,
        piece,
        piece,
    ]
    specs = [whole_spec(o.shape) for o in outs]
    specs[1] = pl.BlockSpec((T, 128), lambda i: (0, jnp.maximum(i - 2 * PAIRS, 0)))
    square = VM((T, T), F32)
    heads = VM((32, T), F32)
    return pl.pallas_call(
        layer_kernel,
        grid=(3 * PAIRS,),
        in_specs=[
            tok,
            tok,
            tok,
            pl.BlockSpec((4, 128), lambda i: (0, lax.rem(i, PAIRS))),
            whole_spec((NH, T)),
            whole_spec((1, NH)),
            whole_spec((1, NH)),
            whole_spec((64, 128)),
            whole_spec((T, 128)),
            whole_spec((T, 128)),
        ]
        + [whole_spec((T, 4 * HEAD_DIM))] * 4
        + [
            pl.BlockSpec((16, WIDTH), lambda i: (T // 16 - 1, 0)),
            pl.BlockSpec(memory_space=pltpu.SMEM),
        ],
        out_specs=specs,
        out_shape=outs,
        scratch_shapes=[
            VM((8, T), F32),
            VM((5, 32, T), F32),
            square,
            VM((3, T, 128), F32),
            VM((NH, T), F32),
            VM((8, 128), F32),
            VM((8 + T, 128), F32),
            VM((T, STATE), BF16),
            VM((T, STATE), BF16),
            VM((WIDTH, T), F32),
            VM((WIDTH, T), F32),
            VM((WIDTH, T), F32),
            VM((WIDTH, T), F32),
            VM((RING, 2, HEAD_DIM, T), BF16),
            VM((RING, 2, HEAD_DIM, T), BF16),
            VM((4 * HEAD_DIM, T), BF16),
            VM((2 * RING, 2, HEAD_DIM, T), BF16),
            VM((RING, 2, HEAD_DIM, T), BF16),
            VM((16, WIDTH), BF16),
            VM((NH, 80, 128), BF16),
            VM((NSEQ, 80, 128), BF16),
            VM((NSEQ, 64, 128), BF16),
            VM((NH, 64, 128), BF16),
            VM((2 * RING, HEAD_DIM, T), F32),
            VM((2 * RING, HEAD_DIM, T), F32),
            VM((RING, HEAD_DIM, T), BF16),
            VM((RING, 2, HEAD_DIM, T), BF16),
            VM((RING, 2, HEAD_DIM, T), BF16),
            VM((RING, HEAD_DIM, T), BF16),
            VM((RING, 2, HEAD_DIM, T), BF16),
            VM((RING, 2, HEAD_DIM, T), BF16),
            VM((4 * HEAD_DIM, T), F32),
            square,
            square,
            square,
            heads,
            heads,
            heads,
            VM((STATE, T), F32),
            VM((STATE, T), F32),
            VM((16 + T, 128), F32),
            VM((16, WIDTH), F32),
            VM((8, WIDTH), F32),
            VM((8, WIDTH), F32),
            VM((BLOCKS, 8, 128), F32),
            VM((NSEQ, 8, 128), F32),
            VM((BLOCKS, 8, 128), F32),
            VM((128, T), BF16),
            VM((4, 128, T), BF16),
            DMA((RING,)), DMA((RING,)), DMA((RING,)), DMA((RING,)), DMA((RING,)), DMA((RING,)),
            DMA, DMA,
            DMA((NSEQ,)), DMA((NSEQ,)), DMA((NSEQ,)), DMA((NSEQ,)),
            DMA((RING,)), DMA((RING,)), DMA((RING,)), DMA((RING,)), DMA((RING,)), DMA((RING,)),
            DMA((BLOCKS,)), DMA((NSEQ,)), DMA((NSEQ,)), DMA((BLOCKS,)),
            DMA((4,)), DMA((4,)), DMA, DMA,
        ],
        compiler_params=pltpu.CompilerParams(
            collective_id=1, has_side_effects=True, vmem_limit_bytes=60 * 1024 * 1024
        ),
        name="layer",
        cost_estimate=pl.CostEstimate(
            flops=6000000000, bytes_accessed=12000000, transcendentals=6000000
        ),
    )(
        conv_input, gate_input, mix_grad, conv_weight, raw, bias, rate, docs, bin_, cout,
        queries, keys, values, attn_grad, conv_input, skip,
    )


def finish_kernel(*refs):
    count = (len(refs) - 4) // 2
    for src, dest in zip(refs[:count], refs[count + 1 : 2 * count + 1]):
        dest[...] = src[...]
    for i in range(3):
        refs[2 * count + 1 + i][...] = refs[count][i : i + 1, 0:NH]


def finish(arrays):
    parts = 7

    def spec(a):
        if a.shape[0] == T and a.shape[1] > 128:
            return pl.BlockSpec((T, a.shape[1] // parts), lambda i: (0, i))
        return whole_spec(a.shape)

    specs = [spec(a) for a in arrays]
    return pl.pallas_call(
        finish_kernel,
        grid=(parts,),
        in_specs=specs,
        out_specs=specs[:-1] + [whole_spec((1, NH))] * 3,
        out_shape=[jax.ShapeDtypeStruct(a.shape, a.dtype) for a in arrays[:-1]]
        + [jax.ShapeDtypeStruct((1, NH), F32)] * 3,
        compiler_params=pltpu.CompilerParams(vmem_limit_bytes=60 * 1024 * 1024),
        name="finish",
        cost_estimate=pl.CostEstimate(flops=1000000, bytes_accessed=7000000, transcendentals=0),
    )(*arrays)


def local(
    queries, keys, values, attn_grad, doc_ids, conv_input, conv_weight, step_raw, step_bias,
    rate_log, skip_gain, input_coeff, output_coeff, gate_input, mix_grad,
):
    outs = layer(
        conv_input, gate_input, mix_grad, conv_weight, step_raw.T, step_bias[None],
        rate_log[None], doc_ids.reshape(64, 128), input_coeff, output_coeff, queries, keys,
        values, attn_grad, skip_gain,
    )
    dconv, dgate, gstep, dw, gin, gout, gq, gk, gv, bias, rate, skip = finish(
        outs[:4] + outs[5:] + outs[4:5]
    )
    return (
        gq, gk, gv, dconv, dgate, gstep.T, gin, gout, dw, bias.reshape(NH), rate.reshape(NH),
        skip.reshape(NH),
    )


def solution(mesh):
    both = P("seq", "head")
    return jax.shard_map(
        local,
        mesh=mesh,
        in_specs=(
            both, both, both, both, P(), both, P(None, "head"), both, P("head"), P("head"),
            P("head"), P("seq", None), P("seq", None), both, both,
        ),
        out_specs=(
            both, both, both, both, both, both, P("seq", None), P("seq", None),
            P(None, "head"), P("head"), P("head"), P("head"),
        ),
        check_vma=False,
    )
```

```python
import jax
import jax.numpy as jnp
from jax import lax
from jax.experimental import pallas as pl
from jax.experimental.pallas import tpu as pltpu
from jax.sharding import PartitionSpec as P

HEAD_DIM = 224
WINDOW = 1024
SSM_HEADS = 112
STATE = 64
GROUPS = 2
T = 256
NH = 28
PAIRS = 14
NSEQ = 32
RING = 4
NEG = -1e30
F32 = jnp.float32
BF16 = jnp.bfloat16
MESH = pl.DeviceIdType.MESH
VM = pltpu.VMEM
SCALE = HEAD_DIM ** (-0.5)
HI = lax.Precision.HIGHEST


def dot(a, b, ca, cb, precision=None):
    return lax.dot_general(
        a, b, (((ca,), (cb,)), ((), ())), preferred_element_type=F32, precision=precision
    )


def sigmoid(v):
    return 1.0 / (1.0 + jnp.exp(-v))


def col_of(row, rows):
    return jnp.transpose(jnp.broadcast_to(row, (rows, row.shape[1])))


DMA = pltpu.SemaphoreType.DMA
WIDTH = NH * 64
BLOCKS = PAIRS + 1
ANY = pl.BlockSpec(memory_space=pl.ANY)


def doc_row(ref, shard):
    safe = jnp.maximum(shard, 0) * 2
    row = jnp.concatenate([ref[pl.ds(safe, 1), :], ref[pl.ds(safe + 1, 1), :]], axis=1)
    return jnp.where(shard < 0, -1.0, row.astype(F32))


def mixer_setup(me, raw_ref, bias_ref, rate_ref, doc_ref, drows, rows, tri, mk, vcol, small):
    base = me - lax.rem(me, RING)
    for c in range(2 * RING):
        drows[c : c + 1, :] = doc_row(doc_ref, base - RING + c)
    doc = doc_row(doc_ref, me)
    prev = doc_row(doc_ref, me - 1)
    small[...] = jnp.zeros_like(small)
    small[0:1, 0:NH] = bias_ref[...]
    small[1:2, 0:NH] = jnp.exp(rate_ref[...])
    bias = col_of(small[0:1, :], 128)[0:NH]
    rate = col_of(small[1:2, :], 128)[0:NH]
    vcol[...] = jnp.concatenate([rate, rate], axis=1)
    rows[...] = jnp.zeros_like(rows)
    step = jnp.log(1.0 + jnp.exp(raw_ref[...] + jnp.concatenate([bias, bias], axis=1)))
    rows[0, 0:NH, :] = step
    rows[1, 0:NH, :] = -step * vcol[...]
    i = lax.broadcasted_iota(jnp.int32, (T, T), 0)
    j = lax.broadcasted_iota(jnp.int32, (T, T), 1)
    tri[...] = jnp.where(i <= j, 1.0, 0.0)
    cum = dot(rows[1], tri[...], 1, 0, HI)
    rows[2] = cum
    rows[3] = jnp.where(doc == prev[:, T - 1 : T], jnp.exp(cum), 0.0)
    rows[4] = jnp.where(
        doc == doc[:, T - 1 : T], jnp.exp(jnp.minimum(cum[:, T - 1 : T] - cum, 0.0)), 0.0
    )
    lane = lax.broadcasted_iota(jnp.int32, (8, T), 1)
    doc8 = jnp.broadcast_to(doc, (8, T))
    prev8 = jnp.broadcast_to(prev, (8, T))
    for k in range(1, 4):
        lag = jnp.where(lane < k, pltpu.roll(prev8, k, 1), pltpu.roll(doc8, k, 1))
        mk[k - 1] = col_of(jnp.where(lag == doc8, 1.0, 0.0)[0:1, :], 128)


def pair_rows(rows, which, pair):
    a = rows[which, pl.ds(2 * pair, 1), :]
    b = rows[which, pl.ds(2 * pair + 1, 1), :]
    return jnp.concatenate(
        [jnp.broadcast_to(a, (64, T)), jnp.broadcast_to(b, (64, T))], axis=0
    )


def group_cols(ref, group):
    v = ref[...].astype(F32)
    return jnp.where(group == 0, v[:, 0:STATE], v[:, STATE:])


def conv_forward(x, tail, w_ref, mk, xs):
    xs[0:8, :] = tail
    xs[8 : 8 + T, :] = x
    pre = w_ref[0:1, :] * x
    for k in range(1, 4):
        pre = pre + w_ref[k : k + 1, :] * (mk[k - 1] * xs[8 - k : 8 - k + T, :])
    return pre


def tail_rows(ref, pair):
    lanes = pl.ds(pl.multiple_of(pair * 128, 128), 128)
    return ref[:, lanes].astype(F32)[8:16]


def seq_copy(src, dst, send, recv, peer):
    return pltpu.make_async_remote_copy(
        src_ref=src,
        dst_ref=dst,
        send_sem=send,
        recv_sem=recv,
        device_id={"seq": peer},
        device_id_type=MESH,
    )


def greet_seq(barrier, me):
    def greet(k, carry):
        peer = lax.rem(me + k, NSEQ)
        pl.semaphore_signal(barrier, inc=1, device_id={"seq": peer}, device_id_type=MESH)
        return carry

    lax.fori_loop(1, NSEQ, greet, 0)


def attention(x_me, kva, qda, drows, dka, dva, dq_out, send_dq, midway):
    dka[...] = jnp.zeros_like(dka)
    dva[...] = jnp.zeros_like(dva)
    row_i = lax.broadcasted_iota(jnp.int32, (T, T), 0)
    col_j = lax.broadcasted_iota(jnp.int32, (T, T), 1)

    def chunk(c, carry):
        pl.when(c == 2)(midway)
        slot = lax.rem(x_me - c + RING, RING)
        qt = qda[slot, 0]
        gt = qda[slot, 1]
        q = jnp.transpose(qt.astype(F32)).astype(BF16)
        g = jnp.transpose(gt.astype(F32)).astype(BF16)
        dq_col = col_of(drows[pl.ds(RING + c, 1), :], 128)
        dq_col = jnp.concatenate([dq_col, dq_col], axis=1)
        scores, slots = [], []
        row_max = None
        for b in range(RING + 1):
            kc = c + b
            slots.append(kc // RING * RING + lax.rem(x_me - kc + 2 * RING, RING))
            s = dot(q, kva[slots[b], 0], 1, 0) * SCALE
            ok = dq_col == drows[pl.ds(kc, 1), :]
            if b == 0:
                ok = ok & (col_j > row_i)
            if b == RING:
                ok = ok & (col_j <= row_i)
            s = jnp.where(ok, s, NEG)
            scores.append(s)
            m = jnp.max(s, axis=1, keepdims=True)
            row_max = m if row_max is None else jnp.maximum(row_max, m)
        row_sum = None
        for b in range(RING + 1):
            e = jnp.exp(scores[b] - row_max)
            scores[b] = e
            r = jnp.sum(e, axis=1, keepdims=True)
            row_sum = r if row_sum is None else row_sum + r
        inv = 1.0 / jnp.maximum(row_sum, 1.0)
        dprobs = []
        delta = None
        for b in range(RING + 1):
            p = scores[b] * inv
            scores[b] = p
            half = p.astype(BF16)
            dp = dot(g, kva[slots[b], 1], 1, 0)
            dprobs.append(dp)
            r = jnp.sum(half.astype(F32) * dp, axis=1, keepdims=True)
            delta = r if delta is None else delta + r
            dva[c + b] = dva[c + b] + dot(gt, half, 1, 0)
        dqt = None
        for b in range(RING + 1):
            ds = (scores[b] * (dprobs[b] - delta)).astype(BF16)
            r = dot(kva[slots[b], 0], ds, 1, 1)
            dqt = r if dqt is None else dqt + r
            dka[c + b] = dka[c + b] + dot(qt, ds, 1, 0)
        k = lax.rem(c - x_me + RING, RING)
        dq_out[k] = (dqt * SCALE).astype(BF16)
        send_dq(k)
        return carry

    lax.fori_loop(0, RING, chunk, 0)


def layer_kernel(
    conv_ref, gate_ref, mix_ref, w_ref, raw_ref, bias_ref, rate_ref, doc_ref, bin_ref, cout_ref,
    q_ref, k_ref, v_ref, do_ref, edge_ref, skip_ref,
    dconv_out, dgate_out, step_out, dw_out, sc_out, gin_out, gout_out, gq_out, gk_out, gv_out,
    drows, rows, tri, mk, vcol, small, xs, bg, cg, act_s, g_s, y_s, ds_s,
    kvp, qdp, tscr, kva, qda, tail_in, pay, inbox, outb, landed,
    dka, dva, dq_out, own_out, back_out, dq_in, own_in, back_in, fscr,
    bias_m, pair_t, dpair, dcum, ddir, dskp, dbt, dct, qs,
    last, spill, spin, red, rinbox, tot, coef_ref, cin,
    hs, hr, ks, kr, qsm, qr, ts, tr, cs1, cr1, cs2, cr2,
    ds_, dr, osm, orr, bs, br, s1, r1, s2, r2, s3, r3, s4, r4,
):
    step_id = pl.program_id(0)
    pair = lax.rem(step_id, PAIRS)
    me = lax.axis_index("seq")
    hd = lax.axis_index("head")
    x_me = lax.rem(me, RING)
    base = me - x_me
    fwd = lax.rem(base + RING, NSEQ)
    bwd = lax.rem(base + NSEQ - RING, NSEQ)

    def near(k):
        return base + lax.rem(x_me + k, RING)

    def halo_copy(k):
        return seq_copy(kva.at[RING + k], kva.at[k], hs.at[k], hr.at[k], fwd + x_me)

    def kv_copy(k):
        return seq_copy(kvp.at[k], kva.at[RING + k], ks.at[k], kr.at[k], near(k))

    def qd_copy(k):
        return seq_copy(qdp.at[k], qda.at[k], qsm.at[k], qr.at[k], near(k))

    def dq_copy(k):
        return seq_copy(dq_out.at[k], dq_in.at[k], ds_.at[k], dr.at[k], near(k))

    def own_copy(k):
        return seq_copy(own_out.at[k], own_in.at[k], osm.at[k], orr.at[k], near(k))

    def back_copy(k):
        return seq_copy(
            back_out.at[k], back_in.at[k], bs.at[k], br.at[k], bwd + lax.rem(x_me + k, RING)
        )

    def first_copy(peer, frm):
        return seq_copy(pay.at[peer], inbox.at[frm], cs1.at[peer], cr1.at[frm], peer)

    def second_copy(peer, frm):
        return seq_copy(outb.at[peer], landed.at[frm], cs2.at[peer], cr2.at[frm], peer)

    tail_copy = seq_copy(edge_ref, tail_in, ts, tr, lax.rem(me + 1, NSEQ))

    @pl.when(step_id == 0)
    def _():
        barrier = pltpu.get_barrier_semaphore()
        greet_seq(barrier, me)
        for k in range(1, 4):
            pl.semaphore_signal(
                barrier, inc=1, device_id={"head": lax.rem(hd + k, 4)}, device_id_type=MESH
            )

        def prepare(src, dest, landing, slot):
            tscr[...] = jnp.transpose(src[...].astype(F32)).astype(BF16)
            for k in range(RING):
                h = lax.rem(x_me + k, RING)
                part = tscr[pl.ds(pl.multiple_of(h * HEAD_DIM, 32), HEAD_DIM), :]
                if k:
                    dest[k, slot] = part
                else:
                    landing[slot] = part

        prepare(k_ref, kvp, kva.at[RING], 0)
        prepare(v_ref, kvp, kva.at[RING], 1)
        pl.semaphore_wait(barrier, NSEQ + 2)
        tail_copy.start()
        halo_copy(0).start()
        for k in (1, 3, 2):
            kv_copy(k).start()
        prepare(q_ref, qdp, qda.at[0], 0)
        prepare(do_ref, qdp, qda.at[0], 1)
        for k in (1, 3, 2):
            qd_copy(k).start()
        red[...] = jnp.zeros_like(red)
        mixer_setup(me, raw_ref, bias_ref, rate_ref, doc_ref, drows, rows, tri, mk, vcol, small)
        group = hd // 2
        bf = group_cols(bin_ref, group)
        cf = group_cols(cout_ref, group)
        bg[...] = bf.astype(BF16)
        cg[...] = cf.astype(BF16)
        thr = rows[3][:, T - 1 : T]
        for e in range(NH):
            t = jnp.broadcast_to(thr[e : e + 1, :], (8, 128))
            hi = t.astype(BF16).astype(F32)
            pay[e, 64:80, :] = jnp.concatenate([hi, t - hi], axis=0).astype(BF16)
        pair_t[...] = dot(bf, cf, 1, 1, HI)
        doc = drows[pl.ds(RING + x_me, 1), :]
        dcol = col_of(doc, 128)
        dcol = jnp.concatenate([dcol, dcol], axis=1)
        bias_m[...] = jnp.where((tri[...] > 0.5) & (dcol == doc), 0.0, NEG)
        for ref in (dpair, dbt, dct, dcum, ddir, dskp, qs):
            ref[...] = jnp.zeros_like(ref)
        tail_copy.wait_recv()

    rows128 = pl.ds(pl.multiple_of(pair * 128, 128), 128)

    @pl.when(step_id < PAIRS)
    def _():
        x = conv_ref[...].astype(F32)
        pre = conv_forward(x, tail_rows(tail_in, pair), w_ref, mk, xs)
        act = pre * sigmoid(pre)
        gate = gate_ref[...].astype(F32)
        g = mix_ref[...].astype(F32) * (gate * sigmoid(gate))
        act_t = jnp.transpose(act)
        g_t = jnp.transpose(g)
        act_s[rows128, :] = act_t
        g_s[rows128, :] = g_t
        st = act_t * (pair_rows(rows, 0, pair) * pair_rows(rows, 4, pair))
        ge = g_t * pair_rows(rows, 3, pair)
        both = jnp.concatenate(
            [dot(st.astype(BF16), bg[...], 1, 0), dot(ge.astype(BF16), cg[...], 1, 0)], axis=1
        ).astype(BF16)
        pay[2 * pair, 0:64, :] = both[0:64]
        pay[2 * pair + 1, 0:64, :] = both[64:128]

    @pl.when(step_id == 7)
    def _():
        for k in (1, 3):
            kv_copy(k).wait_recv()
            halo_copy(k).start()

    @pl.when(step_id == PAIRS - 1)
    def _():
        kv_copy(2).wait_recv()
        halo_copy(2).start()

        def send_first(k, carry):
            peer = lax.rem(me + k, NSEQ)

            @pl.when(peer < NH)
            def _():
                first_copy(peer, me).start()

            return carry

        lax.fori_loop(1, NSEQ, send_first, 0)

    @pl.when(step_id == 2 * PAIRS - 1)
    def _():
        for k in range(1, RING):
            qd_copy(k).wait_recv()
        for k in range(RING):
            halo_copy(k).wait_recv()

        def send_dq(k):
            @pl.when(k > 0)
            def _():
                dq_copy(k).start()

        def midway():
            @pl.when(me < NH)
            def _():
                inbox[me] = pay[me]

                def wait_first(k, carry):
                    first_copy(me, lax.rem(me + k, NSEQ)).wait_recv()
                    return carry

                lax.fori_loop(1, NSEQ, wait_first, 0)
                lane = lax.broadcasted_iota(jnp.int32, (64, 128), 1)

                def gain(s):
                    tail = inbox[s, 64:80, :].astype(F32)
                    return tail[0:1] + tail[8:9]

                def down(s, run):
                    outb[s] = run.astype(BF16)
                    return gain(s) * run + inbox[s, 0:64, :].astype(F32)

                lax.fori_loop(0, NSEQ, down, jnp.zeros((64, 128), F32))

                def up(k, run):
                    s = NSEQ - 1 - k
                    outb[s] = jnp.where(lane < STATE, outb[s].astype(F32), run).astype(BF16)
                    return gain(s) * run + inbox[s, 0:64, :].astype(F32)

                lax.fori_loop(0, NSEQ, up, jnp.zeros((64, 128), F32))

                def send_second(k, carry):
                    second_copy(lax.rem(me + k, NSEQ), me).start()
                    return carry

                lax.fori_loop(1, NSEQ, send_second, 0)
                landed[me] = outb[me]

        attention(x_me, kva, qda, drows, dka, dva, dq_out, send_dq, midway)
        for k in range(RING):
            c = lax.rem(x_me + k, RING)
            back_out[k, 0] = (dka[c] * SCALE).astype(BF16)
            back_out[k, 1] = dva[c].astype(BF16)
            back_copy(k).start()
        for k in range(RING):
            c = lax.rem(x_me + k, RING)
            own_out[k, 0] = (dka[RING + c] * SCALE).astype(BF16)
            own_out[k, 1] = dva[RING + c].astype(BF16)
            if k:
                own_copy(k).start()

    @pl.when(step_id == 2 * PAIRS)
    def _():
        def arrive(k, carry):
            peer = lax.rem(me + k, NSEQ)

            @pl.when(peer < NH)
            def _():
                second_copy(me, peer).wait_recv()

            return carry

        lax.fori_loop(1, NSEQ, arrive, 0)

    @pl.when((step_id >= PAIRS) & (step_id < 2 * PAIRS))
    def _():
        act_t = act_s[rows128, :]
        g_t = g_s[rows128, :]
        s_b = (act_t * pair_rows(rows, 0, pair)).astype(BF16)
        g_b = g_t.astype(BF16)
        ys, dss = [], []
        for a in range(2):
            lo = 64 * a
            h = 2 * pair + a
            cum = rows[2, pl.ds(h, 1), :]
            cc = col_of(cum, 128)
            cc = jnp.concatenate([cc, cc], axis=1)
            w = jnp.exp(jnp.minimum(cum - cc, 0.0) + bias_m[...])
            m = pair_t[...] * w
            mb = m.astype(BF16)
            sh = s_b[lo : lo + 64]
            gh = g_b[lo : lo + 64]
            ys.append(dot(sh, mb, 1, 0))
            dsi = dot(gh, mb, 1, 1)
            dss.append(dsi)
            dm = dot(sh, gh, 0, 0)
            dpair[...] += dm * w
            z = dm * m
            zr = jnp.sum(jnp.transpose(z[:, 0:128] + z[:, 128:]), axis=0, keepdims=True)
            at = act_t[lo : lo + 64]
            dcum[pl.ds(h, 1), :] = jnp.sum(z, axis=0, keepdims=True) - zr
            ddir[pl.ds(h, 1), :] = jnp.sum(dsi * at, axis=0, keepdims=True)
            dskp[pl.ds(h, 1), :] = jnp.sum(g_t[lo : lo + 64] * at, axis=0, keepdims=True)
        y_s[rows128, :] = jnp.concatenate(ys, axis=0)
        ds_s[rows128, :] = jnp.concatenate(dss, axis=0)

    @pl.when(step_id >= 2 * PAIRS)
    def _():
        act_t = act_s[rows128, :]
        g_t = g_s[rows128, :]
        step_p = pair_rows(rows, 0, pair)
        eg_p = pair_rows(rows, 3, pair)
        te_p = pair_rows(rows, 4, pair)
        s_t = act_t * step_p
        state = jnp.concatenate([landed[2 * pair], landed[2 * pair + 1]], axis=0)
        start = state[:, 0:STATE]
        end = state[:, STATE:]
        car = dot(start, cg[...], 1, 1) * eg_p
        dste = dot(end, bg[...], 1, 1) * te_p
        dct[...] += dot(start, (g_t * eg_p).astype(BF16), 0, 0)
        dbt[...] += dot(end, (s_t * te_p).astype(BF16), 0, 0)
        se = start.astype(F32) * end.astype(F32)
        lane = lax.broadcasted_iota(jnp.int32, (1, T), 1)
        skips = []
        for a in range(2):
            part = slice(64 * a, 64 * a + 64)
            h = 2 * pair + a
            v = jnp.sum(s_t[part] * dste[part], axis=0, keepdims=True)
            d = jnp.sum(g_t[part] * car[part], axis=0, keepdims=True) - v
            thr = rows[3, pl.ds(h, 1), :][:, T - 1 : T]
            extra = jnp.sum(v, axis=1, keepdims=True) + thr * jnp.sum(
                jnp.sum(se[part], axis=0, keepdims=True), axis=1, keepdims=True
            )
            dcum[pl.ds(h, 1), :] += d + jnp.where(lane == T - 1, extra, 0.0)
            ddir[pl.ds(h, 1), :] += jnp.sum(dste[part] * act_t[part], axis=0, keepdims=True)
            skips.append(jnp.full((64, T), skip_ref[h], F32))
        skip = jnp.concatenate(skips, axis=0)
        y = jnp.transpose(y_s[rows128, :] + car + skip * act_t)
        dact = jnp.transpose((ds_s[rows128, :] + dste) * step_p + skip * g_t)
        gate = gate_ref[...].astype(F32)
        sg = sigmoid(gate)
        dgate_out[...] = (
            mix_ref[...].astype(F32) * y * (sg * (1.0 + gate * (1.0 - sg)))
        ).astype(BF16)
        x = conv_ref[...].astype(F32)
        pre = conv_forward(x, tail_rows(tail_in, pair), w_ref, mk, xs)
        sp = sigmoid(pre)
        dpre = dact * (sp * (1.0 + pre * (1.0 - sp)))
        dx = None
        for k in range(4):
            q = dpre if k == 0 else dpre * mk[k - 1]
            red[pair, k : k + 1, :] = jnp.sum(q * xs[8 - k : 8 - k + T, :], axis=0, keepdims=True)
            qs[8 : 8 + T, :] = q
            term = w_ref[k : k + 1, :] * qs[k : k + 8 + T, :]
            dx = term if dx is None else dx + term
        spill[:, rows128] = dx[0:8]
        dconv_out[:, rows128] = dx[8:].astype(BF16)
        last[:, rows128] = dx[T - 8 :]

    @pl.when(step_id == 3 * PAIRS - 1)
    def _():
        dld = dot(dcum[...], tri[...], 1, 1, HI)
        rate = vcol[...]
        small[0:1, 0:NH] = bias_ref[...]
        bias = col_of(small[0:1, :], 128)[0:NH]
        v = raw_ref[...] + jnp.concatenate([bias, bias], axis=1)
        dldn = dld[0:NH]
        gs = (ddir[0:NH, :] - dldn * rate) * sigmoid(v)
        step_out[...] = gs
        pick = lax.broadcasted_iota(jnp.int32, (32, 128), 1)
        total = lambda z: jnp.sum(z, axis=1, keepdims=True)
        fscr[...] = jnp.zeros_like(fscr)
        fscr[0:NH, 0:128] = jnp.where(
            pick[0:NH] == 0,
            total(gs),
            jnp.where(pick[0:NH] == 1, total(dldn * rows[1, 0:NH, :]), total(dskp[0:NH, :])),
        )
        red[PAIRS] = jnp.transpose(fscr[0:128, 0:128])[0:8]
        dp = dpair[...].astype(BF16)
        coef_ref[0:STATE] = (dbt[...] + dot(jnp.transpose(cg[...].astype(F32)).astype(BF16), dp, 1, 1)).astype(BF16)
        coef_ref[STATE:] = (dct[...] + dot(jnp.transpose(bg[...].astype(F32)).astype(BF16), dp, 1, 0)).astype(BF16)

        def coef(k, frm):
            return pltpu.make_async_remote_copy(
                src_ref=coef_ref,
                dst_ref=cin.at[frm],
                send_sem=s3.at[k],
                recv_sem=r3.at[frm],
                device_id={"head": lax.rem(hd + k, 4)},
                device_id_type=MESH,
            )

        spill_copy = seq_copy(spill, spin, s4, r4, lax.rem(me + NSEQ - 1, NSEQ))

        def first(block, frm):
            return seq_copy(red.at[block], rinbox.at[frm], s1.at[block], r1.at[frm], 2 * block)

        def second(peer, block):
            return seq_copy(tot.at[block], tot.at[block], s2.at[peer], r2.at[block], peer)

        def send_first(b, carry):
            @pl.when(2 * b != me)
            def _():
                first(b, me).start()

            return carry

        lax.fori_loop(0, BLOCKS, send_first, 0)
        for k in range(1, 4):
            coef(k, hd).start()
        spill_copy.start()
        for k in range(RING):
            if k:
                dq_copy(k).wait_recv()
            h = lax.rem(x_me - k + RING, RING)
            source = dq_in if k else dq_out
            gq_out[pl.ds(pl.multiple_of(h * HEAD_DIM, 32), HEAD_DIM), :] = source[k]
        mine = me // 2
        owner = (me == 2 * mine) & (mine < BLOCKS)

        @pl.when(owner)
        def _():
            rinbox[me] = red[mine]

            def wait_first(k, carry):
                first(mine, lax.rem(me + k, NSEQ)).wait_recv()
                return carry

            lax.fori_loop(1, NSEQ, wait_first, 0)
            tot[mine] = jnp.sum(rinbox[...], axis=0)

            def send_second(k, carry):
                second(lax.rem(me + k, NSEQ), mine).start()
                return carry

            lax.fori_loop(1, NSEQ, send_second, 0)

        for k in range(1, 4):
            coef(k, lax.rem(hd + k, 4)).wait_recv()
        cin[hd] = coef_ref[...]
        g0 = jnp.transpose(cin[0].astype(F32) + cin[1].astype(F32))
        g1 = jnp.transpose(cin[2].astype(F32) + cin[3].astype(F32))
        gin_out[...] = jnp.concatenate([g0[:, 0:STATE], g1[:, 0:STATE]], axis=1)
        gout_out[...] = jnp.concatenate([g0[:, STATE:], g1[:, STATE:]], axis=1)
        spill_copy.wait_recv()
        fixed = jnp.concatenate([last[0:8, :], last[8:16, :] + spin[...]], axis=0)
        dconv_out[T - 16 :, :] = fixed.astype(BF16)
        for k in range(RING):
            back_copy(k).wait_recv()
            if k:
                own_copy(k).wait_recv()
        for slot, dest in ((0, gk_out), (1, gv_out)):
            for k in range(RING):
                mine_k = own_in if k else own_out
                h = lax.rem(x_me - k + RING, RING)
                dest[pl.ds(pl.multiple_of(h * HEAD_DIM, 32), HEAD_DIM), :] = (
                    mine_k[k, slot].astype(F32) + back_in[k, slot].astype(F32)
                ).astype(BF16)

        def wait_second(b, carry):
            @pl.when(2 * b != me)
            def _():
                second(me, b).wait_recv()
                first(b, me).wait_send()

            return carry

        lax.fori_loop(0, BLOCKS, wait_second, 0)
        for p in range(PAIRS):
            dw_out[:, 128 * p : 128 * p + 128] = tot[p, 0:4, :]
        sc_out[...] = tot[PAIRS]

        @pl.when(owner)
        def _():
            def drain(k, carry):
                second(lax.rem(me + k, NSEQ), mine).wait_send()
                return carry

            lax.fori_loop(1, NSEQ, drain, 0)

        for k in range(1, 4):
            coef(k, hd).wait_send()
        spill_copy.wait_send()
        tail_copy.wait_send()
        for k in range(RING):
            halo_copy(k).wait_send()
            back_copy(k).wait_send()
            if k:
                kv_copy(k).wait_send()
                qd_copy(k).wait_send()
                dq_copy(k).wait_send()
                own_copy(k).wait_send()

        def sent_first(k, carry):
            peer = lax.rem(me + k, NSEQ)

            @pl.when(peer < NH)
            def _():
                first_copy(peer, me).wait_send()

            return carry

        lax.fori_loop(1, NSEQ, sent_first, 0)

        @pl.when(me < NH)
        def _():
            def sent_second(k, carry):
                second_copy(lax.rem(me + k, NSEQ), me).wait_send()
                return carry

            lax.fori_loop(1, NSEQ, sent_second, 0)


def whole_spec(shape):
    return pl.BlockSpec(shape, lambda i: (0,) * len(shape))


def layer(
    conv_input, gate_input, mix_grad, conv_weight, raw, bias, rate, docs, bin_, cout,
    queries, keys, values, attn_grad, skip,
):
    tok = pl.BlockSpec((T, 128), lambda i: (0, lax.rem(i, PAIRS)))
    piece = jax.ShapeDtypeStruct((4 * HEAD_DIM, T), BF16)
    outs = [
        jax.ShapeDtypeStruct((T, WIDTH), BF16),
        jax.ShapeDtypeStruct((T, WIDTH), BF16),
        jax.ShapeDtypeStruct((NH, T), F32),
        jax.ShapeDtypeStruct((4, WIDTH), F32),
        jax.ShapeDtypeStruct((8, 128), F32),
        jax.ShapeDtypeStruct((T, 128), F32),
        jax.ShapeDtypeStruct((T, 128), F32),
        piece,
        piece,
        piece,
    ]
    specs = [whole_spec(o.shape) for o in outs]
    specs[1] = pl.BlockSpec((T, 128), lambda i: (0, jnp.maximum(i - 2 * PAIRS, 0)))
    square = VM((T, T), F32)
    heads = VM((32, T), F32)
    return pl.pallas_call(
        layer_kernel,
        grid=(3 * PAIRS,),
        in_specs=[
            tok,
            tok,
            tok,
            pl.BlockSpec((4, 128), lambda i: (0, lax.rem(i, PAIRS))),
            whole_spec((NH, T)),
            whole_spec((1, NH)),
            whole_spec((1, NH)),
            whole_spec((64, 128)),
            whole_spec((T, 128)),
            whole_spec((T, 128)),
        ]
        + [whole_spec((T, 4 * HEAD_DIM))] * 4
        + [
            pl.BlockSpec((16, WIDTH), lambda i: (T // 16 - 1, 0)),
            pl.BlockSpec(memory_space=pltpu.SMEM),
        ],
        out_specs=specs,
        out_shape=outs,
        scratch_shapes=[
            VM((8, T), F32),
            VM((5, 32, T), F32),
            square,
            VM((3, T, 128), F32),
            VM((NH, T), F32),
            VM((8, 128), F32),
            VM((8 + T, 128), F32),
            VM((T, STATE), BF16),
            VM((T, STATE), BF16),
            VM((WIDTH, T), F32),
            VM((WIDTH, T), F32),
            VM((WIDTH, T), F32),
            VM((WIDTH, T), F32),
            VM((RING, 2, HEAD_DIM, T), BF16),
            VM((RING, 2, HEAD_DIM, T), BF16),
            VM((4 * HEAD_DIM, T), BF16),
            VM((2 * RING, 2, HEAD_DIM, T), BF16),
            VM((RING, 2, HEAD_DIM, T), BF16),
            VM((16, WIDTH), BF16),
            VM((NH, 80, 128), BF16),
            VM((NSEQ, 80, 128), BF16),
            VM((NSEQ, 64, 128), BF16),
            VM((NH, 64, 128), BF16),
            VM((2 * RING, HEAD_DIM, T), F32),
            VM((2 * RING, HEAD_DIM, T), F32),
            VM((RING, HEAD_DIM, T), BF16),
            VM((RING, 2, HEAD_DIM, T), BF16),
            VM((RING, 2, HEAD_DIM, T), BF16),
            VM((RING, HEAD_DIM, T), BF16),
            VM((RING, 2, HEAD_DIM, T), BF16),
            VM((RING, 2, HEAD_DIM, T), BF16),
            VM((128, T), F32),
            square,
            square,
            square,
            heads,
            heads,
            heads,
            VM((STATE, T), F32),
            VM((STATE, T), F32),
            VM((16 + T, 128), F32),
            VM((16, WIDTH), F32),
            VM((8, WIDTH), F32),
            VM((8, WIDTH), F32),
            VM((BLOCKS, 8, 128), F32),
            VM((NSEQ, 8, 128), F32),
            VM((BLOCKS, 8, 128), F32),
            VM((128, T), BF16),
            VM((4, 128, T), BF16),
            DMA((RING,)), DMA((RING,)), DMA((RING,)), DMA((RING,)), DMA((RING,)), DMA((RING,)),
            DMA, DMA,
            DMA((NSEQ,)), DMA((NSEQ,)), DMA((NSEQ,)), DMA((NSEQ,)),
            DMA((RING,)), DMA((RING,)), DMA((RING,)), DMA((RING,)), DMA((RING,)), DMA((RING,)),
            DMA((BLOCKS,)), DMA((NSEQ,)), DMA((NSEQ,)), DMA((BLOCKS,)),
            DMA((4,)), DMA((4,)), DMA, DMA,
        ],
        compiler_params=pltpu.CompilerParams(
            collective_id=1, has_side_effects=True, vmem_limit_bytes=60 * 1024 * 1024
        ),
        name="layer",
        cost_estimate=pl.CostEstimate(
            flops=6000000000, bytes_accessed=12000000, transcendentals=6000000
        ),
    )(
        conv_input, gate_input, mix_grad, conv_weight, raw, bias, rate, docs, bin_, cout,
        queries, keys, values, attn_grad, conv_input, skip,
    )


TURNED = (4 * HEAD_DIM, T)


def finish_kernel(*refs):
    count = (len(refs) - 4) // 2
    for src, dest in zip(refs[:count], refs[count + 1 : 2 * count + 1]):
        if src.shape == dest.shape:
            dest[...] = src[...]
        else:
            dest[...] = jnp.transpose(src[...].astype(F32)).astype(BF16)
    for i in range(3):
        refs[2 * count + 1 + i][...] = refs[count][i : i + 1, 0:NH]


def finish(arrays):
    parts = 7

    def spec(a, turn):
        if a.shape == TURNED:
            if turn:
                return pl.BlockSpec((T, a.shape[0] // parts), lambda i: (0, i))
            return pl.BlockSpec((a.shape[0] // parts, T), lambda i: (i, 0))
        if a.shape == (T, WIDTH):
            return pl.BlockSpec((T, WIDTH // parts), lambda i: (0, i))
        return whole_spec(a.shape)

    def result(a):
        shape = (T, 4 * HEAD_DIM) if a.shape == TURNED else a.shape
        return jax.ShapeDtypeStruct(shape, a.dtype)

    return pl.pallas_call(
        finish_kernel,
        grid=(parts,),
        in_specs=[spec(a, False) for a in arrays],
        out_specs=[spec(a, True) for a in arrays[:-1]] + [whole_spec((1, NH))] * 3,
        out_shape=[result(a) for a in arrays[:-1]] + [jax.ShapeDtypeStruct((1, NH), F32)] * 3,
        compiler_params=pltpu.CompilerParams(vmem_limit_bytes=60 * 1024 * 1024),
        name="finish",
        cost_estimate=pl.CostEstimate(flops=1000000, bytes_accessed=7000000, transcendentals=0),
    )(*arrays)


def local(
    queries, keys, values, attn_grad, doc_ids, conv_input, conv_weight, step_raw, step_bias,
    rate_log, skip_gain, input_coeff, output_coeff, gate_input, mix_grad,
):
    outs = layer(
        conv_input, gate_input, mix_grad, conv_weight, step_raw.T, step_bias[None],
        rate_log[None], doc_ids.reshape(64, 128), input_coeff, output_coeff, queries, keys,
        values, attn_grad, skip_gain,
    )
    dconv, dgate, gstep, dw, gin, gout, gq, gk, gv, bias, rate, skip = finish(
        outs[:4] + outs[5:] + outs[4:5]
    )
    return (
        gq, gk, gv, dconv, dgate, gstep.T, gin, gout, dw, bias.reshape(NH), rate.reshape(NH),
        skip.reshape(NH),
    )


def solution(mesh):
    both = P("seq", "head")
    return jax.shard_map(
        local,
        mesh=mesh,
        in_specs=(
            both, both, both, both, P(), both, P(None, "head"), both, P("head"), P("head"),
            P("head"), P("seq", None), P("seq", None), both, both,
        ),
        out_specs=(
            both, both, both, both, both, both, P("seq", None), P("seq", None),
            P(None, "head"), P("head"), P("head"), P("head"),
        ),
        check_vma=False,
    )
```
